32 devices in a mesh: xy: 2 (over core), gz: 4 (over y, x), ta: 4 (over z).
Axes of the slice: x: 2, y: 2, z: 4, core: 2. Of those that a mesh axis runs over, the one named last changes fastest.
Arguments:
- right_side: float32 [2, 4, 4, 128, 128], P('xy', 'gz', 'ta'), may hold values from -40 to 40
- link_blocks: float32 [2, 4, 4, 9, 2, 32, 32, 128], P('xy', 'gz', 'ta'), may hold values from -0.75 to 0.75
Outputs:
- solution: float32 [2, 4, 4, 128, 128], P('xy', 'gz', 'ta')
- residual: float32 [2, 4, 4, 128, 128], P('xy', 'gz', 'ta')
The draws below stay inside these ranges and needn't reach their ends.
All inputs are finite; a program needn't handle non-finite values.
Results may differ from the reference program's by a relative error of at most 0.00018.
Values sent between devices are 32-bit elements; how exact they have to be, the bound alone decides.
No kernel may reach another device: no remote copies, remote signals or barrier semaphores. Data moves between devices by JAX's collectives and lax.ppermute only.
A program may use at most 128 MiB of HBM per device.

```python
import jax
import jax.numpy as jnp
from jax import lax

DOF = 32
RHS = 2
CX = 1
NY = 8
CZ = 2
CT = 8
ITERS = 2
S = 128
VEC = 128
NT = 32
N_XY = 2
N_GZ = 4
N_TA = 4


def draw_right_side(key, part):
    noise_key, rough_key = jax.random.split(jax.random.fold_in(key, 11), 2)
    shape = (N_XY, N_GZ, N_TA, S, VEC)
    time_index = (jnp.arange(N_TA)[:, None] * CT + jnp.arange(S)[None, :] % CT).astype(jnp.float32)
    ramp = jnp.exp(jnp.log(3.0) * time_index / max(NT - 1, 1))
    ramp = ramp[None, None, :, :, None]
    rough = jnp.exp(jax.random.uniform(rough_key, (N_XY, N_GZ, N_TA, S, 1), jnp.float32, -0.8, 0.8))
    base = jax.random.normal(noise_key, shape, jnp.float32)
    return jnp.clip(base * ramp * rough, -40.0, 40.0).astype(jnp.float32)


def steps_of(stream_key, dims, cuts, smallest, largest):
    gain = 1.0
    for position, shards_of in cuts:
        steps = jax.random.uniform(jax.random.fold_in(jax.random.fold_in(stream_key, 6), position), (shards_of,), jnp.float32, smallest / len(cuts), largest / len(cuts))
        gain = gain * jnp.repeat(jnp.exp(steps), dims[position] // shards_of).reshape((-1,) + (1,) * (len(dims) - 1 - position))
    return gain


def gaussian(stream_key, dims, spread, reach, shards=(), held_as=jnp.bfloat16):
    factor_of = steps_of(stream_key, dims, shards, -0.22, 0.18) if shards else 1.0
    drawn = jax.random.normal(stream_key, dims, jnp.float32) * spread * factor_of
    return jnp.minimum(jnp.maximum(drawn, -reach), reach).astype(held_as)


def setup_inputs(seed: int = 0) -> dict:
    arg_keys = jax.random.split(jax.random.key(seed), 3)
    right_side = draw_right_side(jax.random.fold_in(arg_keys[2], 71), 0)
    link_blocks = gaussian(arg_keys[1], (N_XY, N_GZ, N_TA, 9, 2, DOF, DOF, S), (2 * DOF) ** -0.5, 0.75, ((0, 2), (1, 4), (2, 4)), jnp.float32)
    return dict(right_side=right_side, link_blocks=link_blocks)


mass_shift = 4.0
epsilon = 1e-06

def split_parts(joined):
    shaped = joined.reshape(joined.shape[:-1] + (RHS, 2, DOF))
    return (shaped[..., 0, :], shaped[..., 1, :])

def join_parts(real, imaginary):
    stacked = jnp.stack((real, imaginary), -2)
    return stacked.reshape(stacked.shape[:-3] + (-1,))

def column_sums(values):
    folded = lax.optimization_barrier(jnp.sum(values, axis=-1))
    return lax.optimization_barrier(jnp.sum(folded.reshape(-1, folded.shape[-1]), axis=0))

def to_lattice(joined):
    shaped = joined.reshape(N_XY, N_GZ, N_TA, CX, NY, CZ, CT, joined.shape[-1])
    moved = jnp.transpose(shaped, (0, 3, 4, 1, 5, 2, 6, 7))
    return moved.reshape(N_XY * CX, NY, N_GZ * CZ, N_TA * CT, joined.shape[-1])

def to_blocks(lattice):
    shaped = lattice.reshape(N_XY, CX, NY, N_GZ, CZ, N_TA, CT, lattice.shape[-1])
    moved = jnp.transpose(shaped, (0, 3, 5, 1, 2, 4, 6, 7))
    return moved.reshape(N_XY, N_GZ, N_TA, CX * NY * CZ * CT, lattice.shape[-1])

def single(blocks, field):
    return jnp.einsum('...cds,...srd->...src', blocks, field, precision=lax.Precision.HIGHEST)

def apply_operator(link_blocks, real, imaginary):
    lattice = to_lattice(join_parts(real, imaginary))
    shifted_operator = [lattice]
    for axis_number in range(4):
        shifted_operator.append(jnp.roll(lattice, -1, axis_number))
        shifted_operator.append(jnp.roll(lattice, 1, axis_number))
    out_real = mass_shift * real
    output_imaginary = mass_shift * imaginary
    for level in range(9):
        near_real, near_imag = split_parts(to_blocks(shifted_operator[level]))
        blocks_real = link_blocks[:, :, :, level, 0]
        blocks_imag = link_blocks[:, :, :, level, 1]
        out_real = out_real + single(blocks_real, near_real) - single(blocks_imag, near_imag)
        output_imaginary = output_imaginary + single(blocks_real, near_imag) + single(blocks_imag, near_real)
    return (out_real, output_imaginary)

def solve_positive_definite(matrix, target):
    size = matrix.shape[0]
    lower = {}
    for row in range(size):
        for col in range(row + 1):
            value = matrix[row, col]
            for inner in range(col):
                value = value - lower[row, inner] * lower[col, inner]
            if row == col:
                lower[row, row] = jnp.sqrt(value)
            else:
                lower[row, col] = value / lower[col, col]
    forward = []
    for row in range(size):
        value = target[row]
        for inner in range(row):
            value = value - lower[row, inner] * forward[inner]
        forward.append(value / lower[row, row])
    answer = [None] * size
    for row in reversed(range(size)):
        value = forward[row]
        for inner in range(row + 1, size):
            value = value - lower[inner, row] * answer[inner]
        answer[row] = value / lower[row, row]
    return jnp.stack(answer)

def least_squares(hessenberg_real, hessenberg_imaginary, beta):
    exact_answer_vector = lax.Precision.HIGHEST
    gram_matrix_real = jnp.einsum('sxm,szm->xzm', hessenberg_real, hessenberg_real, precision=exact_answer_vector) + jnp.einsum('sxm,szm->xzm', hessenberg_imaginary, hessenberg_imaginary, precision=exact_answer_vector)
    gram_matrix_imaginary = jnp.einsum('sxm,szm->xzm', hessenberg_real, hessenberg_imaginary, precision=exact_answer_vector) - jnp.einsum('sxm,szm->xzm', hessenberg_imaginary, hessenberg_real, precision=exact_answer_vector)
    upper = jnp.concatenate((gram_matrix_real, -gram_matrix_imaginary), 1)
    bottom = jnp.concatenate((gram_matrix_imaginary, gram_matrix_real), 1)
    system = jnp.concatenate((upper, bottom), 0)
    target = jnp.concatenate((beta[None, :] * hessenberg_real[0], -beta[None, :] * hessenberg_imaginary[0]), 0)
    answer = solve_positive_definite(system, target)
    return (answer[:ITERS], answer[ITERS:])

def reference(right_side, link_blocks):
    rhs_real, rhs_imag = split_parts(right_side)
    beta = jnp.sqrt(column_sums(rhs_real * rhs_real + rhs_imag * rhs_imag) + epsilon)
    basis = [(rhs_real / beta[:, None], rhs_imag / beta[:, None])]
    hessenberg_real = jnp.zeros((ITERS + 1, ITERS, RHS), jnp.float32)
    hessenberg_imaginary = jnp.zeros((ITERS + 1, ITERS, RHS), jnp.float32)
    for step in range(ITERS):
        work_real, work_imag = apply_operator(link_blocks, basis[step][0], basis[step][1])
        proj_real = jnp.stack([column_sums(vector[0] * work_real + vector[1] * work_imag) for vector in basis])
        proj_imag = jnp.stack([column_sums(vector[0] * work_imag - vector[1] * work_real) for vector in basis])
        for index in range(len(basis)):
            coef_real = proj_real[index][:, None]
            coef_imag = proj_imag[index][:, None]
            vector = basis[index]
            work_real = work_real - (coef_real * vector[0] - coef_imag * vector[1])
            work_imag = work_imag - (coef_real * vector[1] + coef_imag * vector[0])
        norm = jnp.sqrt(column_sums(work_real * work_real + work_imag * work_imag) + epsilon)
        hessenberg_real = hessenberg_real.at[:step + 1, step].set(proj_real)
        hessenberg_imaginary = hessenberg_imaginary.at[:step + 1, step].set(proj_imag)
        hessenberg_real = hessenberg_real.at[step + 1, step].set(norm)
        basis.append((work_real / norm[:, None], work_imag / norm[:, None]))
    coef_real, coef_imag = least_squares(hessenberg_real, hessenberg_imaginary, beta)
    sol_real = jnp.zeros_like(rhs_real)
    sol_imag = jnp.zeros_like(rhs_imag)
    for index in range(ITERS):
        weight_real = coef_real[index][:, None]
        weight_imag = coef_imag[index][:, None]
        sol_real = sol_real + weight_real * basis[index][0] - weight_imag * basis[index][1]
        sol_imag = sol_imag + weight_real * basis[index][1] + weight_imag * basis[index][0]
    image_real, image_imag = apply_operator(link_blocks, sol_real, sol_imag)
    return (join_parts(sol_real, sol_imag), join_parts(rhs_real - image_real, rhs_imag - image_imag))
```

```python
import jax
import jax.numpy as jnp
from jax import lax
from jax.experimental import pallas as pl
from jax.experimental.pallas import tpu as pltpu
from jax.sharding import PartitionSpec as P

DOF = 32
RHS = 2
CX = 1
NY = 8
CZ = 2
CT = 8
S = CX * NY * CZ * CT
VEC = RHS * 2 * DOF
SUB = 8
TILES = DOF // SUB
AXES = ("xy", "gz", "ta")

mass_shift = 4.0
epsilon = 1e-06
f32 = jnp.float32

VMEM_SPEC = pl.BlockSpec(memory_space=pltpu.VMEM)
PARAMS = pltpu.CompilerParams(vmem_limit_bytes=12 * 1024 * 1024)

LOCAL_DIRS = ((0, (0,)), (1, (3,)), (2, (4,)))


def call(body, outs, scratch=(), name=None):
    return pl.pallas_call(
        body,
        out_shape=[jax.ShapeDtypeStruct(o, f32) for o in outs],
        out_specs=[VMEM_SPEC] * len(outs),
        scratch_shapes=list(scratch),
        compiler_params=PARAMS,
        name=name,
    )


def write_faces(src_ref, zlo_ref, zhi_ref, tlo_ref, thi_ref):
    pairs = src_ref[...].reshape(NY, CZ * CT, VEC)
    zlo_ref[...] = pairs[:, :CT].reshape(NY * CT, VEC)
    zhi_ref[...] = pairs[:, (CZ - 1) * CT :].reshape(NY * CT, VEC)
    rows = S // CT
    tlo_ref[...] = src_ref[pl.ds(0, rows, stride=CT), :]
    thi_ref[...] = src_ref[pl.ds(CT - 1, rows, stride=CT), :]


FACES = ((NY * CT, VEC), (NY * CT, VEC), (S // CT, VEC), (S // CT, VEC))


def faces_body(src_ref, zlo_ref, zhi_ref, tlo_ref, thi_ref):
    write_faces(src_ref, zlo_ref, zhi_ref, tlo_ref, thi_ref)


def multiply(fields, links, groups, red, out, add=None):
    def chunk(cb, carry):
        acc = [None] * (2 * RHS * SUB)
        for field, dirs in groups:
            for tile in range(TILES):
                x = [
                    fields[field, part * DOF + tile * SUB : part * DOF + (tile + 1) * SUB, :]
                    for part in range(2 * RHS)
                ]
                rows = pl.ds(tile * SUB, SUB)
                for c in range(SUB):
                    lr = links[dirs[0], 0, cb * SUB + c, rows, :]
                    li = links[dirs[0], 1, cb * SUB + c, rows, :]
                    for k in dirs[1:]:
                        lr = lr + links[k, 0, cb * SUB + c, rows, :]
                        li = li + links[k, 1, cb * SUB + c, rows, :]
                    for r in range(RHS):
                        re = lr * x[2 * r] - li * x[2 * r + 1]
                        im = lr * x[2 * r + 1] + li * x[2 * r]
                        for part, value in ((2 * r, re), (2 * r + 1, im)):
                            slot = part * SUB + c
                            acc[slot] = value if acc[slot] is None else acc[slot] + value
        for slot, value in enumerate(acc):
            red[slot * SUB : (slot + 1) * SUB, :] = value
        for part in range(2 * RHS):
            total = red[pl.ds(part * SUB * SUB, SUB, stride=SUB), :]
            for d in range(1, SUB):
                total = total + red[pl.ds(part * SUB * SUB + d, SUB, stride=SUB), :]
            where = pl.ds(pl.multiple_of(part * DOF + cb * SUB, SUB), SUB)
            if add is not None:
                total = total + add[where, :]
            out[where, :] = total
        return carry

    lax.fori_loop(0, TILES, chunk, 0)


RED = pltpu.VMEM((2 * RHS * SUB * SUB, S), f32)


def local_body(src, links, src_t, part, fields, red):
    own = src[...]
    step = CZ * CT
    fields[0] = own.T
    fields[1] = jnp.concatenate([own[step:], own[:step]], axis=0).T
    fields[2] = jnp.concatenate([own[S - step :], own[: S - step]], axis=0).T
    src_t[...] = fields[0]
    multiply(fields, links, LOCAL_DIRS, red, part)


def remote_groups(n_x):
    return ((0, (1, 2)),) if n_x == 1 else ((0, (1,)), (1, (2,)))


def gather_fields(src, xs, zp, zm, tp, tm, fields, pad):
    own = src[...].reshape(NY, CZ * CT, VEC)
    at = 0
    for x in xs:
        fields[at] = x[...].T
        at += 1
    zplus = jnp.concatenate([own[:, CT:], zp[...].reshape(NY, CT, VEC)], axis=1)
    fields[at] = zplus.reshape(S, VEC).T
    zminus = jnp.concatenate([zm[...].reshape(NY, CT, VEC), own[:, : (CZ - 1) * CT]], axis=1)
    fields[at + 1] = zminus.reshape(S, VEC).T
    rows = S // CT
    for i in range(rows):
        pad[2 * i * CT : (2 * i + 1) * CT, :] = src[i * CT : (i + 1) * CT, :]
    pad[pl.ds(CT, rows, stride=2 * CT), :] = tp[...]
    tplus = jnp.concatenate(
        [pad[2 * i * CT + 1 : (2 * i + 1) * CT + 1, :] for i in range(rows)], axis=0
    )
    fields[at + 2] = tplus.T
    for i in range(rows):
        pad[(2 * i + 1) * CT : (2 * i + 2) * CT, :] = src[i * CT : (i + 1) * CT, :]
    pad[pl.ds(CT - 1, rows, stride=2 * CT), :] = tm[...]
    tminus = jnp.concatenate(
        [pad[(2 * i + 1) * CT - 1 : (2 * i + 2) * CT - 1, :] for i in range(rows)], axis=0
    )
    fields[at + 3] = tminus.T


def remote_dirs(n_x):
    return remote_groups(n_x) + tuple((n_x + i, (5 + i,)) for i in range(4))


def remote_scratch(n_x):
    return (pltpu.VMEM((n_x + 4, VEC, S), f32), RED, pltpu.VMEM((2 * S, VEC), f32))


def first_apply(n_x):
    def body(src, *refs):
        xs = refs[:n_x]
        zp, zm, tp, tm, links, part = refs[n_x : n_x + 6]
        out_t, out, zlo, zhi, tlo, thi, fields, red, pad = refs[n_x + 6 :]
        gather_fields(src, xs, zp, zm, tp, tm, fields, pad)
        multiply(fields, links, remote_dirs(n_x), red, out_t, part)
        out[...] = out_t[...].T
        write_faces(out, zlo, zhi, tlo, thi)

    return call(body, ((VEC, S), (S, VEC)) + FACES, remote_scratch(n_x), "first_apply")


def halves(ref, r):
    top = 2 * r * DOF
    return ref[top : top + DOF, :], ref[top + DOF : top + 2 * DOF, :]


def column(values):
    return jnp.sum(values, axis=0, keepdims=True)


def square(u):
    return [column(u[0] * u[0] + u[1] * u[1])]


def inner(u, w):
    return [column(u[0] * w[0] + u[1] * w[1]), column(u[0] * w[1] - u[1] * w[0])]


TERMS = 9


def second_apply(n_x, devices):
    def body(src, *refs):
        xs = refs[:n_x]
        zp, zm, tp, tm, links, part, first_t, zero_t = refs[n_x : n_x + 8]
        out_t, sums, fields, red, pad, table = refs[n_x + 8 :]
        gather_fields(src, xs, zp, zm, tp, tm, fields, pad)
        multiply(fields, links, remote_dirs(n_x), red, out_t, part)
        table[...] = jnp.zeros_like(table)
        for r in range(RHS):
            b, u, w = halves(zero_t, r), halves(first_t, r), halves(out_t, r)
            rows = square(b) + inner(b, u) + square(u) + inner(b, w) + inner(u, w) + square(w)
            for i, row in enumerate(rows):
                table[r * TERMS + i : r * TERMS + i + 1, :] = row
        total = column(table[...].T)
        sums[...] = jnp.broadcast_to(total[None], sums.shape)

    return call(
        body,
        ((VEC, S), (devices, 1, S)),
        remote_scratch(n_x) + (pltpu.VMEM((S, S), f32),),
        "second_apply",
    )


def times(u, w):
    return (u[0] * w[0] - u[1] * w[1], u[0] * w[1] + u[1] * w[0])


def conj_times(u, w):
    return (u[0] * w[0] + u[1] * w[1], u[0] * w[1] - u[1] * w[0])


def plus(u, w):
    return (u[0] + w[0], u[1] + w[1])


def minus(u, w):
    return (u[0] - w[0], u[1] - w[1])


def scaled(s, u):
    return (s * u[0], s * u[1])


def norm2(u):
    return u[0] * u[0] + u[1] * u[1]


def coefficients(bb, bu, uu, bw, uw, ww):
    m = mass_shift
    inv = 1.0 / (bb + epsilon)
    tiny = epsilon * inv
    h00 = scaled(inv, (bu[0] + m * bb, bu[1]))
    q = (inv * bu[0] - m * tiny, inv * bu[1])
    pp = uu - 2.0 * conj_times(q, bu)[0] + norm2(q) * bb
    pp = jnp.maximum(pp, 0.0)
    s = pp * inv
    eta = s + epsilon
    bp = scaled(tiny, (bu[0] + m * bb, bu[1]))
    blp = minus(bw, times(q, bu))
    plp = minus(minus(uw, scaled(uu, q)), conj_times(q, bw))
    plp = plus(plp, scaled(norm2(q), bu))
    lplp = ww - 2.0 * conj_times(q, uw)[0] + norm2(q) * uu
    h01 = scaled(inv, plus(scaled(m, bp), blp))
    h11 = scaled(inv, (m * pp + plp[0], plp[1]))
    dp = inv * (m * m * pp + 2.0 * m * plp[0] + lplp)
    inv_eta = 1.0 / eta
    a00 = norm2(h00) + eta
    a01 = plus(conj_times(h00, h01), h11)
    cross = times(conj_times(h01, h11), bp)[0] * inv * inv_eta
    a11 = dp - norm2(h01) * tiny - norm2(h11) * (epsilon * inv_eta * inv_eta)
    a11 = a11 + 2.0 * cross + eta * epsilon
    inv00 = 1.0 / a00
    pivot = jnp.maximum(a11 - norm2(a01) * inv00, eta * epsilon)
    r0 = (h00[0], -h00[1])
    r1 = (h01[0], -h01[1])
    t = scaled(1.0 / pivot, minus(r1, scaled(inv00, conj_times(a01, r0))))
    y = scaled(inv00, minus(r0, times(a01, t)))
    return minus(y, times(t, q)), t


def final_body(sums, zero_t, first_t, second_t, sol, res, stage):
    total = jnp.sum(sums[...], axis=0)
    stage[...] = jnp.broadcast_to(total, stage.shape).T
    sol_rows = []
    res_rows = []
    for r in range(RHS):
        v = [stage[r * TERMS + i : r * TERMS + i + 1, :] for i in range(TERMS)]
        a, t = coefficients(v[0], (v[1], v[2]), v[3], (v[4], v[5]), (v[6], v[7]), v[8])
        b, u, w = halves(zero_t, r), halves(first_t, r), halves(second_t, r)
        x = plus(times(a, b), times(t, u))
        image = plus(scaled(mass_shift, x), plus(times(a, u), times(t, w)))
        left = minus(b, image)
        sol_rows += list(x)
        res_rows += list(left)
    sol[...] = jnp.concatenate(sol_rows, axis=0).T
    res[...] = jnp.concatenate(res_rows, axis=0).T


def from_next(value, axis):
    n = lax.axis_size(axis)
    return lax.ppermute(value, axis, [((i + 1) % n, i) for i in range(n)])


def from_last(value, axis):
    n = lax.axis_size(axis)
    return lax.ppermute(value, axis, [(i, (i + 1) % n) for i in range(n)])


def halo(value, faces):
    zlo, zhi, tlo, thi = faces
    xs = [from_next(value, "xy")]
    if lax.axis_size("xy") > 2:
        xs.append(from_last(value, "xy"))
    return xs, (
        from_next(zlo, "gz"),
        from_last(zhi, "gz"),
        from_next(tlo, "ta"),
        from_last(thi, "ta"),
    )


def shards(right_side, link_blocks):
    b = right_side.reshape(S, VEC)
    links = link_blocks.reshape(link_blocks.shape[3:])
    links = pltpu.with_memory_space_constraint(links, pltpu.VMEM)
    n_x = 1 if lax.axis_size("xy") == 2 else 2
    devices = lax.axis_size("xy") * lax.axis_size("gz") * lax.axis_size("ta")
    local = call(
        local_body, ((VEC, S), (VEC, S)), (pltpu.VMEM((3, VEC, S), f32), RED), "local_apply"
    )

    faces = call(faces_body, FACES, (), "faces")(b)
    xs, edges = halo(b, faces)
    b_t, part = local(b, links)
    u_t, u, *faces = first_apply(n_x)(b, *xs, *edges, links, part)
    xs, edges = halo(u, faces)
    _, part = local(u, links)
    w_t, sums = second_apply(n_x, devices)(u, *xs, *edges, links, part, u_t, b_t)
    sums = lax.all_to_all(sums, AXES, 0, 0)
    sol, res = call(final_body, ((S, VEC), (S, VEC)), (pltpu.VMEM((S, S), f32),), "final")(
        sums, b_t, u_t, w_t
    )
    return sol.reshape(right_side.shape), res.reshape(right_side.shape)


def solution(mesh):
    return jax.shard_map(
        shards,
        mesh=mesh,
        in_specs=(
            P("xy", "gz", "ta", None, None),
            P("xy", "gz", "ta", None, None, None, None, None),
        ),
        out_specs=(P("xy", "gz", "ta", None, None), P("xy", "gz", "ta", None, None)),
        check_vma=False,
    )
```

```python
import jax
import jax.numpy as jnp
from jax import lax
from jax.experimental import pallas as pl
from jax.experimental.pallas import tpu as pltpu
from jax.sharding import PartitionSpec as P


DOF = 32
RHS = 2
CX = 1
NY = 8
CZ = 2
CT = 8
S = CX * NY * CZ * CT
VEC = RHS * 2 * DOF
SUB = 8
TILES = DOF // SUB
AXES = ("xy", "gz", "ta")

mass_shift = 4.0
epsilon = 1e-06
f32 = jnp.float32
FIRST_COST = 20_000_000_000

VMEM_SPEC = pl.BlockSpec(memory_space=pltpu.VMEM)
PARAMS = pltpu.CompilerParams(vmem_limit_bytes=12 * 1024 * 1024)


def call(body, outs, scratch=(), cost=None):
    if cost is not None:
        cost = pl.CostEstimate(flops=cost, bytes_accessed=0, transcendentals=0)
    return pl.pallas_call(
        body,
        out_shape=[jax.ShapeDtypeStruct(o, f32) for o in outs],
        out_specs=[VMEM_SPEC] * len(outs),
        scratch_shapes=list(scratch),
        compiler_params=PARAMS,
        cost_estimate=cost,
    )


def swap_halves(axis, first, second):
    odd = lax.axis_index(axis) % 2 == 1
    return jnp.where(odd, second, first), jnp.where(odd, first, second)


def write_faces(src_ref, za_ref, zb_ref, ta_ref, tb_ref):
    pairs = src_ref[...].reshape(NY, CZ * CT, VEC)
    low = pairs[:, :CT].reshape(NY * CT, VEC)
    high = pairs[:, (CZ - 1) * CT :].reshape(NY * CT, VEC)
    za_ref[...], zb_ref[...] = swap_halves("gz", high, low)
    rows = S // CT
    low = src_ref[pl.ds(0, rows, stride=CT), :]
    high = src_ref[pl.ds(CT - 1, rows, stride=CT), :]
    ta_ref[...], tb_ref[...] = swap_halves("ta", high, low)


FACES = ((NY * CT, VEC), (NY * CT, VEC), (S // CT, VEC), (S // CT, VEC))


def faces_body(src_ref, *outs):
    write_faces(src_ref, *outs)


def multiply(fields, links, groups, red, out, add=None):
    def chunk(cb, carry):
        acc = [None] * (2 * RHS * SUB)
        for field, dirs in groups:
            for tile in range(TILES):
                x = [
                    fields[field, part * DOF + tile * SUB : part * DOF + (tile + 1) * SUB, :]
                    for part in range(2 * RHS)
                ]
                rows = pl.ds(tile * SUB, SUB)
                for c in range(SUB):
                    lr = links[dirs[0], 0, cb * SUB + c, rows, :]
                    li = links[dirs[0], 1, cb * SUB + c, rows, :]
                    for k in dirs[1:]:
                        lr = lr + links[k, 0, cb * SUB + c, rows, :]
                        li = li + links[k, 1, cb * SUB + c, rows, :]
                    for r in range(RHS):
                        re = lr * x[2 * r] - li * x[2 * r + 1]
                        im = lr * x[2 * r + 1] + li * x[2 * r]
                        for part, value in ((2 * r, re), (2 * r + 1, im)):
                            slot = part * SUB + c
                            acc[slot] = value if acc[slot] is None else acc[slot] + value
        for slot, value in enumerate(acc):
            red[slot * SUB : (slot + 1) * SUB, :] = value
        for part in range(2 * RHS):
            total = red[pl.ds(part * SUB * SUB, SUB, stride=SUB), :]
            for d in range(1, SUB):
                total = total + red[pl.ds(part * SUB * SUB + d, SUB, stride=SUB), :]
            where = pl.ds(pl.multiple_of(part * DOF + cb * SUB, SUB), SUB)
            if add is not None:
                total = total + add[where, :]
            out[where, :] = total
        return carry

    lax.fori_loop(0, TILES, chunk, 0)


RED = pltpu.VMEM((2 * RHS * SUB * SUB, S), f32)


def local_dirs(n_x):
    dirs = ((0, (0,)), (1, (3,)), (2, (4,)))
    if n_x == 1:
        return dirs + ((3, (1, 2)),)
    return dirs + ((3, (1,)), (4, (2,)))


def local_apply(n_x, with_copy):
    def body(src, *refs):
        xs = [x[...] for x in refs[:n_x]]
        if n_x == 2:
            xs = swap_halves("xy", *xs)
        links, part = refs[n_x : n_x + 2]
        fields, red = refs[-2:]
        own = src[...]
        step = CZ * CT
        fields[0] = own.T
        fields[1] = jnp.concatenate([own[step:], own[:step]], axis=0).T
        fields[2] = jnp.concatenate([own[S - step :], own[: S - step]], axis=0).T
        for i, x in enumerate(xs):
            fields[3 + i] = x.T
        if with_copy:
            refs[n_x + 2][...] = fields[0]
        multiply(fields, links, local_dirs(n_x), red, part)

    outs = ((VEC, S),) * (2 if with_copy else 1)
    return call(body, outs, (pltpu.VMEM((3 + n_x, VEC, S), f32), RED))


REMOTE_DIRS = tuple((i, (5 + i,)) for i in range(4))


def gather_fields(src, za, zb, ta, tb, fields, pad):
    own = src[...].reshape(NY, CZ * CT, VEC)
    zp, zm = swap_halves("gz", za[...], zb[...])
    tp, tm = swap_halves("ta", ta[...], tb[...])
    zplus = jnp.concatenate([own[:, CT:], zp.reshape(NY, CT, VEC)], axis=1)
    fields[0] = zplus.reshape(S, VEC).T
    zminus = jnp.concatenate([zm.reshape(NY, CT, VEC), own[:, : (CZ - 1) * CT]], axis=1)
    fields[1] = zminus.reshape(S, VEC).T
    rows = S // CT
    for i in range(rows):
        pad[2 * i * CT : (2 * i + 1) * CT, :] = src[i * CT : (i + 1) * CT, :]
    pad[pl.ds(CT, rows, stride=2 * CT), :] = tp
    tplus = jnp.concatenate(
        [pad[2 * i * CT + 1 : (2 * i + 1) * CT + 1, :] for i in range(rows)], axis=0
    )
    fields[2] = tplus.T
    for i in range(rows):
        pad[(2 * i + 1) * CT : (2 * i + 2) * CT, :] = src[i * CT : (i + 1) * CT, :]
    pad[pl.ds(CT - 1, rows, stride=2 * CT), :] = tm
    tminus = jnp.concatenate(
        [pad[(2 * i + 1) * CT - 1 : (2 * i + 2) * CT - 1, :] for i in range(rows)], axis=0
    )
    fields[3] = tminus.T


REMOTE_SCRATCH = (pltpu.VMEM((4, VEC, S), f32), RED, pltpu.VMEM((2 * S, VEC), f32))


def first_body(src, za, zb, ta, tb, links, part, out_t, out, *refs):
    faces, (fields, red, pad) = refs[:4], refs[4:]
    gather_fields(src, za, zb, ta, tb, fields, pad)
    multiply(fields, links, REMOTE_DIRS, red, out_t, part)
    out[...] = out_t[...].T
    write_faces(out, *faces)


def halves(ref, r):
    top = 2 * r * DOF
    return ref[top : top + DOF, :], ref[top + DOF : top + 2 * DOF, :]


def column(values):
    return jnp.sum(values, axis=0, keepdims=True)


def square(u):
    return [column(u[0] * u[0] + u[1] * u[1])]


def inner(u, w):
    return [column(u[0] * w[0] + u[1] * w[1]), column(u[0] * w[1] - u[1] * w[0])]


TERMS = 9


def second_body(src, za, zb, ta, tb, links, part, first_t, zero_t, *refs):
    out_t, sums, fields, red, pad, table = refs
    gather_fields(src, za, zb, ta, tb, fields, pad)
    multiply(fields, links, REMOTE_DIRS, red, out_t, part)
    table[...] = jnp.zeros_like(table)
    for r in range(RHS):
        b, u, w = halves(zero_t, r), halves(first_t, r), halves(out_t, r)
        rows = square(b) + inner(b, u) + square(u) + inner(b, w) + inner(u, w) + square(w)
        for i, row in enumerate(rows):
            table[r * TERMS + i : r * TERMS + i + 1, :] = row
    total = column(table[...].T)
    sums[...] = jnp.broadcast_to(total[None], sums.shape)


def times(u, w):
    return (u[0] * w[0] - u[1] * w[1], u[0] * w[1] + u[1] * w[0])


def conj_times(u, w):
    return (u[0] * w[0] + u[1] * w[1], u[0] * w[1] - u[1] * w[0])


def plus(u, w):
    return (u[0] + w[0], u[1] + w[1])


def minus(u, w):
    return (u[0] - w[0], u[1] - w[1])


def scaled(s, u):
    return (s * u[0], s * u[1])


def norm2(u):
    return u[0] * u[0] + u[1] * u[1]


def coefficients(bb, bu, uu, bw, uw, ww):
    m = mass_shift
    inv = 1.0 / (bb + epsilon)
    tiny = epsilon * inv
    h00 = scaled(inv, (bu[0] + m * bb, bu[1]))
    q = (inv * bu[0] - m * tiny, inv * bu[1])
    pp = uu - 2.0 * conj_times(q, bu)[0] + norm2(q) * bb
    pp = jnp.maximum(pp, 0.0)
    s = pp * inv
    eta = s + epsilon
    bp = scaled(tiny, (bu[0] + m * bb, bu[1]))
    blp = minus(bw, times(q, bu))
    plp = minus(minus(uw, scaled(uu, q)), conj_times(q, bw))
    plp = plus(plp, scaled(norm2(q), bu))
    lplp = ww - 2.0 * conj_times(q, uw)[0] + norm2(q) * uu
    h01 = scaled(inv, plus(scaled(m, bp), blp))
    h11 = scaled(inv, (m * pp + plp[0], plp[1]))
    dp = inv * (m * m * pp + 2.0 * m * plp[0] + lplp)
    inv_eta = 1.0 / eta
    a00 = norm2(h00) + eta
    a01 = plus(conj_times(h00, h01), h11)
    cross = times(conj_times(h01, h11), bp)[0] * inv * inv_eta
    a11 = dp - norm2(h01) * tiny - norm2(h11) * (epsilon * inv_eta * inv_eta)
    a11 = a11 + 2.0 * cross + eta * epsilon
    inv00 = 1.0 / a00
    pivot = jnp.maximum(a11 - norm2(a01) * inv00, eta * epsilon)
    r0 = (h00[0], -h00[1])
    r1 = (h01[0], -h01[1])
    t = scaled(1.0 / pivot, minus(r1, scaled(inv00, conj_times(a01, r0))))
    y = scaled(inv00, minus(r0, times(a01, t)))
    return minus(y, times(t, q)), t


def final_body(sums, zero_t, first_t, second_t, sol, res, stage):
    total = jnp.sum(sums[...], axis=0)
    stage[...] = jnp.broadcast_to(total, stage.shape).T
    sol_rows = []
    res_rows = []
    for r in range(RHS):
        v = [stage[r * TERMS + i : r * TERMS + i + 1, :] for i in range(TERMS)]
        a, t = coefficients(v[0], (v[1], v[2]), v[3], (v[4], v[5]), (v[6], v[7]), v[8])
        b, u, w = halves(zero_t, r), halves(first_t, r), halves(second_t, r)
        x = plus(times(a, b), times(t, u))
        image = plus(scaled(mass_shift, x), plus(times(a, u), times(t, w)))
        left = minus(b, image)
        sol_rows += list(x)
        res_rows += list(left)
    sol[...] = jnp.concatenate(sol_rows, axis=0).T
    res[...] = jnp.concatenate(res_rows, axis=0).T


def exchange(value, axis, offset):
    n = lax.axis_size(axis)
    if n % 2:
        raise ValueError("odd axis " + axis)
    return lax.ppermute(
        value, axis, [(i, (i + 1 if (i - offset) % 2 == 0 else i - 1) % n) for i in range(n)]
    )


def halo(value, faces):
    za, zb, ta, tb = faces
    sent = {}
    plan = [("xa", value, "xy", 0)]
    if lax.axis_size("xy") > 2:
        plan.append(("xb", value, "xy", 1))
    plan += [("tb", tb, "ta", 1), ("zb", zb, "gz", 1), ("ta", ta, "ta", 0), ("za", za, "gz", 0)]
    for key, piece, axis, offset in plan:
        sent[key] = exchange(piece, axis, offset)
    xs = [sent[k] for k in ("xa", "xb") if k in sent]
    return xs, [sent[k] for k in ("za", "zb", "ta", "tb")]


def shards(right_side, link_blocks):
    b = right_side.reshape(S, VEC)
    links = link_blocks.reshape(link_blocks.shape[3:])
    links = pltpu.with_memory_space_constraint(links, pltpu.VMEM)
    n_x = 1 if lax.axis_size("xy") == 2 else 2
    devices = lax.axis_size("xy") * lax.axis_size("gz") * lax.axis_size("ta")

    faces = call(faces_body, FACES, (), FIRST_COST)(b)
    xs, edges = halo(b, faces)
    part, b_t = local_apply(n_x, True)(b, *xs, links)
    u_t, u, *faces = call(
        first_body, ((VEC, S), (S, VEC)) + FACES, REMOTE_SCRATCH
    )(b, *edges, links, part)
    xs, edges = halo(u, faces)
    (part,) = local_apply(n_x, False)(u, *xs, links)
    w_t, sums = call(
        second_body, ((VEC, S), (devices, 1, S)), REMOTE_SCRATCH + (pltpu.VMEM((S, S), f32),)
    )(u, *edges, links, part, u_t, b_t)
    sums = lax.all_to_all(sums, AXES, 0, 0)
    sol, res = call(final_body, ((S, VEC), (S, VEC)), (pltpu.VMEM((S, S), f32),))(
        sums, b_t, u_t, w_t
    )
    return sol.reshape(right_side.shape), res.reshape(right_side.shape)


def solution(mesh):
    return jax.shard_map(
        shards,
        mesh=mesh,
        in_specs=(
            P("xy", "gz", "ta", None, None),
            P("xy", "gz", "ta", None, None, None, None, None),
        ),
        out_specs=(P("xy", "gz", "ta", None, None), P("xy", "gz", "ta", None, None)),
        check_vma=False,
    )
```

```python
import jax
import jax.numpy as jnp
from jax import lax
from jax.experimental import pallas as pl
from jax.experimental.pallas import tpu as pltpu
from jax.sharding import PartitionSpec as P


DOF = 32
RHS = 2
CX = 1
NY = 8
CZ = 2
CT = 8
S = CX * NY * CZ * CT
VEC = RHS * 2 * DOF
SUB = 8
TILES = DOF // SUB
AXES = ("xy", "gz", "ta")

mass_shift = 4.0
epsilon = 1e-06
f32 = jnp.float32
ORDER = ("tb", "x", "zb", "ta", "za")
FIRST_COST = 20_000_000_000

VMEM_SPEC = pl.BlockSpec(memory_space=pltpu.VMEM)
PARAMS = pltpu.CompilerParams(vmem_limit_bytes=12 * 1024 * 1024)


def call(body, outs, scratch=(), cost=None):
    if cost is not None:
        cost = pl.CostEstimate(flops=cost, bytes_accessed=0, transcendentals=0)
    return pl.pallas_call(
        body,
        out_shape=[jax.ShapeDtypeStruct(o, f32) for o in outs],
        out_specs=[VMEM_SPEC] * len(outs),
        scratch_shapes=list(scratch),
        compiler_params=PARAMS,
        cost_estimate=cost,
    )


def swap_halves(axis, first, second):
    odd = lax.axis_index(axis) % 2 == 1
    return jnp.where(odd, second, first), jnp.where(odd, first, second)


def write_faces(src_ref, za_ref, zb_ref, ta_ref, tb_ref):
    pairs = src_ref[...].reshape(NY, CZ * CT, VEC)
    low = pairs[:, :CT].reshape(NY * CT, VEC)
    high = pairs[:, (CZ - 1) * CT :].reshape(NY * CT, VEC)
    za_ref[...], zb_ref[...] = swap_halves("gz", high, low)
    rows = S // CT
    low = src_ref[pl.ds(0, rows, stride=CT), :]
    high = src_ref[pl.ds(CT - 1, rows, stride=CT), :]
    ta_ref[...], tb_ref[...] = swap_halves("ta", high, low)


FACES = ((NY * CT, VEC), (NY * CT, VEC), (S // CT, VEC), (S // CT, VEC))


def faces_body(src_ref, *outs):
    write_faces(src_ref, *outs)


def multiply(fields, links, groups, red, out, add=None):
    def chunk(cb, carry):
        acc = [None] * (2 * RHS * SUB)
        for field, dirs in groups:
            for tile in range(TILES):
                x = [
                    fields[field, part * DOF + tile * SUB : part * DOF + (tile + 1) * SUB, :]
                    for part in range(2 * RHS)
                ]
                rows = pl.ds(tile * SUB, SUB)
                for c in range(SUB):
                    lr = links[dirs[0], 0, cb * SUB + c, rows, :]
                    li = links[dirs[0], 1, cb * SUB + c, rows, :]
                    for k in dirs[1:]:
                        lr = lr + links[k, 0, cb * SUB + c, rows, :]
                        li = li + links[k, 1, cb * SUB + c, rows, :]
                    for r in range(RHS):
                        re = lr * x[2 * r] - li * x[2 * r + 1]
                        im = lr * x[2 * r + 1] + li * x[2 * r]
                        for part, value in ((2 * r, re), (2 * r + 1, im)):
                            slot = part * SUB + c
                            acc[slot] = value if acc[slot] is None else acc[slot] + value
        for slot, value in enumerate(acc):
            red[slot * SUB : (slot + 1) * SUB, :] = value
        for part in range(2 * RHS):
            total = red[pl.ds(part * SUB * SUB, SUB, stride=SUB), :]
            for d in range(1, SUB):
                total = total + red[pl.ds(part * SUB * SUB + d, SUB, stride=SUB), :]
            where = pl.ds(pl.multiple_of(part * DOF + cb * SUB, SUB), SUB)
            if add is not None:
                total = total + add[where, :]
            out[where, :] = total
        return carry

    lax.fori_loop(0, TILES, chunk, 0)


RED = pltpu.VMEM((2 * RHS * SUB * SUB, S), f32)


def assemble_z(own, edge, plus):
    blocks = own.reshape(NY, CZ * CT, VEC)
    edge = edge.reshape(NY, CT, VEC)
    up = jnp.concatenate([blocks[:, CT:], edge], axis=1)
    down = jnp.concatenate([edge, blocks[:, : (CZ - 1) * CT]], axis=1)
    return jnp.where(plus, up, down).reshape(S, VEC).T


def assemble_t(own, edge, plus, pad):
    rows = S // CT
    step = 3 * CT
    for i in range(rows):
        pad[i * step + CT : i * step + 2 * CT, :] = own[i * CT : (i + 1) * CT, :]
    pad[pl.ds(CT - 1, rows, stride=step), :] = edge
    pad[pl.ds(2 * CT, rows, stride=step), :] = edge
    pieces = []
    for i in range(rows):
        up = pad[i * step + CT + 1 : i * step + 2 * CT + 1, :]
        down = pad[i * step + CT - 1 : i * step + 2 * CT - 1, :]
        pieces.append(jnp.where(plus, up, down))
    return jnp.concatenate(pieces, axis=0).T


PAD = pltpu.VMEM((3 * S, VEC), f32)


def edge_fields(own, z_edge, t_edge, which, fields, at, pad):
    dirs = []
    for k, axis in enumerate(("gz", "ta")):
        down = (lax.axis_index(axis) + which) % 2
        if axis == "gz":
            fields[at] = assemble_z(own, z_edge, down == 0)
        else:
            fields[at + 1] = assemble_t(own, t_edge, down == 0, pad)
        dirs.append((at + k, (5 + 2 * k + down,)))
    return tuple(dirs)


def local_part(n_x, with_copy):
    def body(src, *refs):
        xs = [x[...] for x in refs[:n_x]]
        if n_x == 2:
            xs = swap_halves("xy", *xs)
        links, part = refs[n_x : n_x + 2]
        fields, red = refs[-2:]
        own = src[...]
        step = CZ * CT
        fields[0] = own.T
        fields[1] = jnp.concatenate([own[step:], own[:step]], axis=0).T
        fields[2] = jnp.concatenate([own[S - step :], own[: S - step]], axis=0).T
        for i, x in enumerate(xs):
            fields[3 + i] = x.T
        if with_copy:
            refs[n_x + 2][...] = fields[0]
        dirs = ((0, (0,)), (1, (3,)), (2, (4,)))
        dirs += ((3, (1, 2)),) if n_x == 1 else ((3, (1,)), (4, (2,)))
        multiply(fields, links, dirs, red, part)

    outs = ((VEC, S),) * (2 if with_copy else 1)
    return call(body, outs, (pltpu.VMEM((3 + n_x, VEC, S), f32), RED))


LAST_SCRATCH = (pltpu.VMEM((2, VEC, S), f32), RED, PAD)


def edge_part(which, src, ze, te, links, part, out_t, fields, red, pad):
    dirs = edge_fields(src[...], ze[...], te[...], which, fields, 0, pad)
    multiply(fields, links, dirs, red, out_t, part)


def edge_body(*refs):
    edge_part(1, *refs)


def add_edges(*args):
    return call(edge_body, ((VEC, S),), LAST_SCRATCH)(*args)[0]


def first_body(src, za, ta, links, part, out_t, out, *refs):
    faces, scratch = refs[:4], refs[4:]
    edge_part(0, src, za, ta, links, part, out_t, *scratch)
    out[...] = out_t[...].T
    write_faces(out, *faces)


def halves(ref, r):
    top = 2 * r * DOF
    return ref[top : top + DOF, :], ref[top + DOF : top + 2 * DOF, :]


def column(values):
    return jnp.sum(values, axis=0, keepdims=True)


def square(u):
    return [column(u[0] * u[0] + u[1] * u[1])]


def inner(u, w):
    return [column(u[0] * w[0] + u[1] * w[1]), column(u[0] * w[1] - u[1] * w[0])]


TERMS = 9


def second_body(src, za, ta, links, part, first_t, zero_t, out_t, sums, *refs):
    table, scratch = refs[-1], refs[:-1]
    edge_part(0, src, za, ta, links, part, out_t, *scratch)
    table[...] = jnp.zeros_like(table)
    for r in range(RHS):
        b, u, w = halves(zero_t, r), halves(first_t, r), halves(out_t, r)
        rows = square(b) + inner(b, u) + square(u) + inner(b, w) + inner(u, w) + square(w)
        for i, row in enumerate(rows):
            table[r * TERMS + i : r * TERMS + i + 1, :] = row
    total = column(table[...].T)
    sums[...] = jnp.broadcast_to(total[None], sums.shape)


def times(u, w):
    return (u[0] * w[0] - u[1] * w[1], u[0] * w[1] + u[1] * w[0])


def conj_times(u, w):
    return (u[0] * w[0] + u[1] * w[1], u[0] * w[1] - u[1] * w[0])


def plus(u, w):
    return (u[0] + w[0], u[1] + w[1])


def minus(u, w):
    return (u[0] - w[0], u[1] - w[1])


def scaled(s, u):
    return (s * u[0], s * u[1])


def norm2(u):
    return u[0] * u[0] + u[1] * u[1]


def coefficients(bb, bu, uu, bw, uw, ww):
    m = mass_shift
    inv = 1.0 / (bb + epsilon)
    tiny = epsilon * inv
    h00 = scaled(inv, (bu[0] + m * bb, bu[1]))
    q = (inv * bu[0] - m * tiny, inv * bu[1])
    pp = uu - 2.0 * conj_times(q, bu)[0] + norm2(q) * bb
    pp = jnp.maximum(pp, 0.0)
    s = pp * inv
    eta = s + epsilon
    bp = scaled(tiny, (bu[0] + m * bb, bu[1]))
    blp = minus(bw, times(q, bu))
    plp = minus(minus(uw, scaled(uu, q)), conj_times(q, bw))
    plp = plus(plp, scaled(norm2(q), bu))
    lplp = ww - 2.0 * conj_times(q, uw)[0] + norm2(q) * uu
    h01 = scaled(inv, plus(scaled(m, bp), blp))
    h11 = scaled(inv, (m * pp + plp[0], plp[1]))
    dp = inv * (m * m * pp + 2.0 * m * plp[0] + lplp)
    inv_eta = 1.0 / eta
    a00 = norm2(h00) + eta
    a01 = plus(conj_times(h00, h01), h11)
    cross = times(conj_times(h01, h11), bp)[0] * inv * inv_eta
    a11 = dp - norm2(h01) * tiny - norm2(h11) * (epsilon * inv_eta * inv_eta)
    a11 = a11 + 2.0 * cross + eta * epsilon
    inv00 = 1.0 / a00
    pivot = jnp.maximum(a11 - norm2(a01) * inv00, eta * epsilon)
    r0 = (h00[0], -h00[1])
    r1 = (h01[0], -h01[1])
    t = scaled(1.0 / pivot, minus(r1, scaled(inv00, conj_times(a01, r0))))
    y = scaled(inv00, minus(r0, times(a01, t)))
    return minus(y, times(t, q)), t


def final_body(sums, zero_t, first_t, second_t, sol, res, stage):
    total = jnp.sum(sums[...], axis=0)
    stage[...] = jnp.broadcast_to(total, stage.shape).T
    sol_rows = []
    res_rows = []
    for r in range(RHS):
        v = [stage[r * TERMS + i : r * TERMS + i + 1, :] for i in range(TERMS)]
        a, t = coefficients(v[0], (v[1], v[2]), v[3], (v[4], v[5]), (v[6], v[7]), v[8])
        b, u, w = halves(zero_t, r), halves(first_t, r), halves(second_t, r)
        x = plus(times(a, b), times(t, u))
        image = plus(scaled(mass_shift, x), plus(times(a, u), times(t, w)))
        left = minus(b, image)
        sol_rows += list(x)
        res_rows += list(left)
    sol[...] = jnp.concatenate(sol_rows, axis=0).T
    res[...] = jnp.concatenate(res_rows, axis=0).T


def exchange(value, axis, offset):
    n = lax.axis_size(axis)
    if n % 2:
        raise ValueError("odd axis " + axis)
    return lax.ppermute(
        value, axis, [(i, (i + 1 if (i - offset) % 2 == 0 else i - 1) % n) for i in range(n)]
    )


def halo(value, faces):
    za, zb, ta, tb = faces
    sent = {}
    plan = {
        "tb": [("tb", tb, "ta", 1)],
        "zb": [("zb", zb, "gz", 1)],
        "za": [("za", za, "gz", 0)],
        "ta": [("ta", ta, "ta", 0)],
        "x": [("xa", value, "xy", 0)],
    }
    if lax.axis_size("xy") > 2:
        plan["x"].append(("xb", value, "xy", 1))
    plan = [entry for key in ORDER for entry in plan[key]]
    for key, piece, axis, offset in plan:
        sent[key] = exchange(piece, axis, offset)
    xs = [sent[k] for k in ("xa", "xb") if k in sent]
    return xs, [sent["zb"], sent["tb"]], [sent["za"], sent["ta"]]


def shards(right_side, link_blocks):
    b = right_side.reshape(S, VEC)
    links = link_blocks.reshape(link_blocks.shape[3:])
    links = pltpu.with_memory_space_constraint(links, pltpu.VMEM)
    n_x = 1 if lax.axis_size("xy") == 2 else 2
    devices = lax.axis_size("xy") * lax.axis_size("gz") * lax.axis_size("ta")

    faces = call(faces_body, FACES, (), FIRST_COST)(b)
    xs, early, late = halo(b, faces)
    part, b_t = local_part(n_x, True)(b, *xs, links)
    part = add_edges(b, *early, links, part)
    u_t, u, *faces = call(
        first_body, ((VEC, S), (S, VEC)) + FACES, LAST_SCRATCH
    )(b, *late, links, part)
    xs, early, late = halo(u, faces)
    (part,) = local_part(n_x, False)(u, *xs, links)
    part = add_edges(u, *early, links, part)
    w_t, sums = call(
        second_body,
        ((VEC, S), (devices, 1, S)),
        LAST_SCRATCH + (pltpu.VMEM((S, S), f32),),
    )(u, *late, links, part, u_t, b_t)
    sums = lax.all_to_all(sums, AXES, 0, 0)
    sol, res = call(final_body, ((S, VEC), (S, VEC)), (pltpu.VMEM((S, S), f32),))(
        sums, b_t, u_t, w_t
    )
    return sol.reshape(right_side.shape), res.reshape(right_side.shape)


def solution(mesh):
    return jax.shard_map(
        shards,
        mesh=mesh,
        in_specs=(
            P("xy", "gz", "ta", None, None),
            P("xy", "gz", "ta", None, None, None, None, None),
        ),
        out_specs=(P("xy", "gz", "ta", None, None), P("xy", "gz", "ta", None, None)),
        check_vma=False,
    )
```

```python
import jax
import jax.numpy as jnp
from jax import lax
from jax.experimental import pallas as pl
from jax.experimental.pallas import tpu as pltpu
from jax.sharding import PartitionSpec as P


DOF = 32
RHS = 2
CX = 1
NY = 8
CZ = 2
CT = 8
S = CX * NY * CZ * CT
VEC = RHS * 2 * DOF
SUB = 8
TILES = DOF // SUB
AXES = ("xy", "gz", "ta")

mass_shift = 4.0
epsilon = 1e-06
f32 = jnp.float32
EDGES = (("tb", "zb", "ta", "za"), ("tb", "zb", "ta", "za"))
ORDERS = (("tb", "x", "zb", "ta", "za"), ("tb", "x", "zb", "ta", "za"))
FIRST_COST = 20_000_000_000

PARAMS = pltpu.CompilerParams(vmem_limit_bytes=12 * 1024 * 1024)


def call(body, outs, scratch=(), cost=None, space=pltpu.VMEM):
    if cost is not None:
        cost = pl.CostEstimate(flops=cost, bytes_accessed=0, transcendentals=0)
    return pl.pallas_call(
        body,
        out_shape=[jax.ShapeDtypeStruct(o, f32) for o in outs],
        out_specs=[pl.BlockSpec(memory_space=space)] * len(outs),
        scratch_shapes=list(scratch),
        compiler_params=PARAMS,
        cost_estimate=cost,
    )


def swap_halves(axis, first, second):
    odd = lax.axis_index(axis) % 2 == 1
    return jnp.where(odd, second, first), jnp.where(odd, first, second)


def write_faces(src_ref, za_ref, zb_ref, ta_ref, tb_ref):
    pairs = src_ref[...].reshape(NY, CZ * CT, VEC)
    low = pairs[:, :CT].reshape(NY * CT, VEC)
    high = pairs[:, (CZ - 1) * CT :].reshape(NY * CT, VEC)
    za_ref[...], zb_ref[...] = swap_halves("gz", high, low)
    rows = S // CT
    low = src_ref[pl.ds(0, rows, stride=CT), :]
    high = src_ref[pl.ds(CT - 1, rows, stride=CT), :]
    ta_ref[...], tb_ref[...] = swap_halves("ta", high, low)


FACES = ((NY * CT, VEC), (NY * CT, VEC), (S // CT, VEC), (S // CT, VEC))


def faces_body(src_ref, *outs):
    write_faces(src_ref, *outs)


def multiply(fields, links, groups, red, out, add=None, unroll=False):
    def chunk(cb, carry):
        acc = [None] * (2 * RHS * SUB)
        for field, dirs in groups:
            for tile in range(TILES):
                x = [
                    fields[field, part * DOF + tile * SUB : part * DOF + (tile + 1) * SUB, :]
                    for part in range(2 * RHS)
                ]
                rows = pl.ds(tile * SUB, SUB)
                for c in range(SUB):
                    lr = links[dirs[0], 0, cb * SUB + c, rows, :]
                    li = links[dirs[0], 1, cb * SUB + c, rows, :]
                    for k in dirs[1:]:
                        lr = lr + links[k, 0, cb * SUB + c, rows, :]
                        li = li + links[k, 1, cb * SUB + c, rows, :]
                    for r in range(RHS):
                        re = lr * x[2 * r] - li * x[2 * r + 1]
                        im = lr * x[2 * r + 1] + li * x[2 * r]
                        for part, value in ((2 * r, re), (2 * r + 1, im)):
                            slot = part * SUB + c
                            acc[slot] = value if acc[slot] is None else acc[slot] + value
        for slot, value in enumerate(acc):
            red[slot * SUB : (slot + 1) * SUB, :] = value
        for part in range(2 * RHS):
            total = red[pl.ds(part * SUB * SUB, SUB, stride=SUB), :]
            for d in range(1, SUB):
                total = total + red[pl.ds(part * SUB * SUB + d, SUB, stride=SUB), :]
            where = pl.ds(pl.multiple_of(part * DOF + cb * SUB, SUB), SUB)
            if add is not None:
                total = total + add[where, :]
            out[where, :] = total
        return carry

    lax.fori_loop(0, TILES, chunk, 0, unroll=unroll)


RED = pltpu.VMEM((2 * RHS * SUB * SUB, S), f32)


def assemble_z(own, edge, plus):
    blocks = own.reshape(NY, CZ * CT, VEC)
    edge = edge.reshape(NY, CT, VEC)
    up = jnp.concatenate([blocks[:, CT:], edge], axis=1)
    down = jnp.concatenate([edge, blocks[:, : (CZ - 1) * CT]], axis=1)
    return jnp.where(plus, up, down).reshape(S, VEC).T


def assemble_t(own, edge, plus, pad):
    rows = S // CT
    step = 3 * CT
    for i in range(rows):
        pad[i * step + CT : i * step + 2 * CT, :] = own[i * CT : (i + 1) * CT, :]
    pad[pl.ds(CT - 1, rows, stride=step), :] = edge
    pad[pl.ds(2 * CT, rows, stride=step), :] = edge
    pieces = []
    for i in range(rows):
        up = pad[i * step + CT + 1 : i * step + 2 * CT + 1, :]
        down = pad[i * step + CT - 1 : i * step + 2 * CT - 1, :]
        pieces.append(jnp.where(plus, up, down))
    return jnp.concatenate(pieces, axis=0).T


PAD = pltpu.VMEM((3 * S, VEC), f32)


def edge_part(edge, src, piece, links, part, out_t, fields, red, pad):
    axis, which = ("gz" if edge[0] == "z" else "ta"), (1 if edge[1] == "b" else 0)
    down = (lax.axis_index(axis) + which) % 2
    if axis == "gz":
        fields[0] = assemble_z(src[...], piece[...], down == 0)
        first = 5
    else:
        fields[0] = assemble_t(src[...], piece[...], down == 0, pad)
        first = 7
    multiply(fields, links, ((0, (first + down,)),), red, out_t, part, True)


EDGE_SCRATCH = (pltpu.VMEM((1, VEC, S), f32), RED, PAD)


def add_edge(edge, *args):
    body = lambda *refs: edge_part(edge, *refs)
    return call(body, ((VEC, S),), EDGE_SCRATCH)(*args)[0]


def rotated(v):
    lane = lax.broadcasted_iota(jnp.int32, v.shape, 1)
    real = (lane // DOF) % 2 == 0
    return jnp.where(real, -pltpu.roll(v, VEC - DOF, 1), pltpu.roll(v, DOF, 1))


def local_part(n_x, second):
    def body(src, *refs):
        xs = [x[...] for x in refs[:n_x]]
        if n_x == 2:
            xs = swap_halves("xy", *xs)
        links = refs[n_x]
        fields, red = refs[-2:]
        own = src[...]
        step = CZ * CT
        fields[0] = own.T
        fields[1] = jnp.concatenate([own[step:], own[:step]], axis=0).T
        fields[2] = jnp.concatenate([own[S - step :], own[: S - step]], axis=0).T
        for i, x in enumerate(xs):
            fields[3 + i] = x.T
        if second:
            zero, part, rot_zero, rot_first = refs[n_x + 1 : n_x + 5]
            rot_zero[...] = rotated(zero[...])
            rot_first[...] = rotated(own)
        else:
            part, src_t = refs[n_x + 1 : n_x + 3]
            src_t[...] = fields[0]
        dirs = ((0, (0,)), (1, (3,)), (2, (4,)))
        dirs += ((3, (1, 2)),) if n_x == 1 else ((3, (1,)), (4, (2,)))
        multiply(fields, links, dirs, red, part)

    outs = ((VEC, S),) + (((S, VEC),) * 2 if second else ((VEC, S),))
    return call(body, outs, (pltpu.VMEM((3 + n_x, VEC, S), f32), RED))


def first_body(edge):
    def body(src, piece, links, part, out_t, out, *refs):
        faces, scratch = refs[:4], refs[4:]
        edge_part(edge, src, piece, links, part, out_t, *scratch)
        out[...] = out_t[...].T
        write_faces(out, *faces)

    return body


def halves(ref, r):
    top = 2 * r * DOF
    return ref[top : top + DOF, :], ref[top + DOF : top + 2 * DOF, :]


def column(values):
    return jnp.sum(values, axis=0, keepdims=True)


def square(u):
    return [column(u[0] * u[0] + u[1] * u[1])]


def inner(u, w):
    return [column(u[0] * w[0] + u[1] * w[1]), column(u[0] * w[1] - u[1] * w[0])]


TERMS = 9
TABLE = pltpu.VMEM((-(-TERMS * RHS // SUB) * SUB, S), f32)


def slots(shape):
    row = lax.broadcasted_iota(jnp.int32, shape, 0)
    lane = lax.broadcasted_iota(jnp.int32, shape, 1)
    r = sum((row >= TERMS * k).astype(jnp.int32) for k in range(1, RHS))
    return (lane == (row - r * TERMS) * SUB + r) & (row < RHS * TERMS)


def second_body(edge, src, piece, links, part, first_t, zero_t, out_t, sums, *refs):
    table, scratch = refs[-1], refs[:-1]
    edge_part(edge, src, piece, links, part, out_t, *scratch)
    table[...] = jnp.zeros_like(table)
    for r in range(RHS):
        b, u, w = halves(zero_t, r), halves(first_t, r), halves(out_t, r)
        rows = square(b) + inner(b, u) + square(u) + inner(b, w) + inner(u, w) + square(w)
        for i, row in enumerate(rows):
            table[r * TERMS + i : r * TERMS + i + 1, :] = row
    total = jnp.sum(table[...], axis=1, keepdims=True)
    total = column(jnp.where(slots(table.shape), total, 0.0))
    sums[...] = jnp.broadcast_to(total[None], sums.shape)


def times(u, w):
    return (u[0] * w[0] - u[1] * w[1], u[0] * w[1] + u[1] * w[0])


def conj_times(u, w):
    return (u[0] * w[0] + u[1] * w[1], u[0] * w[1] - u[1] * w[0])


def plus(u, w):
    return (u[0] + w[0], u[1] + w[1])


def minus(u, w):
    return (u[0] - w[0], u[1] - w[1])


def scaled(s, u):
    return (s * u[0], s * u[1])


def norm2(u):
    return u[0] * u[0] + u[1] * u[1]


def coefficients(bb, bu, uu, bw, uw, ww):
    m = mass_shift
    inv = 1.0 / (bb + epsilon)
    tiny = epsilon * inv
    h00 = scaled(inv, (bu[0] + m * bb, bu[1]))
    q = (inv * bu[0] - m * tiny, inv * bu[1])
    pp = uu - 2.0 * conj_times(q, bu)[0] + norm2(q) * bb
    pp = jnp.maximum(pp, 0.0)
    s = pp * inv
    eta = s + epsilon
    bp = scaled(tiny, (bu[0] + m * bb, bu[1]))
    blp = minus(bw, times(q, bu))
    plp = minus(minus(uw, scaled(uu, q)), conj_times(q, bw))
    plp = plus(plp, scaled(norm2(q), bu))
    lplp = ww - 2.0 * conj_times(q, uw)[0] + norm2(q) * uu
    h01 = scaled(inv, plus(scaled(m, bp), blp))
    h11 = scaled(inv, (m * pp + plp[0], plp[1]))
    dp = inv * (m * m * pp + 2.0 * m * plp[0] + lplp)
    inv_eta = 1.0 / eta
    a00 = norm2(h00) + eta
    a01 = plus(conj_times(h00, h01), h11)
    cross = times(conj_times(h01, h11), bp)[0] * inv * inv_eta
    a11 = dp - norm2(h01) * tiny - norm2(h11) * (epsilon * inv_eta * inv_eta)
    a11 = a11 + 2.0 * cross + eta * epsilon
    inv00 = 1.0 / a00
    pivot = jnp.maximum(a11 - norm2(a01) * inv00, eta * epsilon)
    r0 = (h00[0], -h00[1])
    r1 = (h01[0], -h01[1])
    t = scaled(1.0 / pivot, minus(r1, scaled(inv00, conj_times(a01, r0))))
    y = scaled(inv00, minus(r0, times(a01, t)))
    return minus(y, times(t, q)), t


def per_lane(rows):
    lane = lax.broadcasted_iota(jnp.int32, (1, VEC), 1)
    out = rows[0:1, :]
    for r in range(1, RHS):
        out = jnp.where(lane < 2 * r * DOF, out, rows[r : r + 1, :])
    return out


def final_body(sums, zero, rot_zero, zero_t, first, rot_first, first_t, second_t, *refs):
    sol, res, sol_stage, res_stage, sems = refs
    total = jnp.broadcast_to(jnp.sum(sums[...], axis=0), (SUB, S))
    row = lax.broadcasted_iota(jnp.int32, (SUB, S), 0)
    lane = lax.broadcasted_iota(jnp.int32, (SUB, S), 1)
    v = []
    for i in range(TERMS):
        value = jnp.sum(jnp.where(lane == i * SUB + row, total, 0.0), axis=1, keepdims=True)
        v.append(jnp.broadcast_to(value, (SUB, S)))
    a, t = coefficients(v[0], (v[1], v[2]), v[3], (v[4], v[5]), (v[6], v[7]), v[8])
    sol_stage[...] = (
        per_lane(a[0]) * zero[...]
        + per_lane(a[1]) * rot_zero[...]
        + per_lane(t[0]) * first[...]
        + per_lane(t[1]) * rot_first[...]
    )
    sol_copy = pltpu.make_async_copy(sol_stage, sol, sems.at[0])
    sol_copy.start()
    keep = (1.0 - mass_shift * a[0], -mass_shift * a[1])
    mixed = plus(scaled(mass_shift, t), a)
    rows = []
    for r in range(RHS):
        at = lambda u: (u[0][r : r + 1, :], u[1][r : r + 1, :])
        b, u, w = halves(zero_t, r), halves(first_t, r), halves(second_t, r)
        rows += list(minus(minus(times(at(keep), b), times(at(mixed), u)), times(at(t), w)))
    res_stage[...] = jnp.concatenate(rows, axis=0).T
    res_copy = pltpu.make_async_copy(res_stage, res, sems.at[1])
    res_copy.start()
    sol_copy.wait()
    res_copy.wait()


FINAL_SCRATCH = (
    pltpu.VMEM((S, VEC), f32),
    pltpu.VMEM((S, VEC), f32),
    pltpu.SemaphoreType.DMA((2,)),
)


def exchange(value, axis, offset):
    n = lax.axis_size(axis)
    if n % 2:
        raise ValueError("odd axis " + axis)
    return lax.ppermute(
        value, axis, [(i, (i + 1 if (i - offset) % 2 == 0 else i - 1) % n) for i in range(n)]
    )


def halo(value, faces, order):
    za, zb, ta, tb = faces
    sent = {}
    plan = {
        "tb": [("tb", tb, "ta", 1)],
        "zb": [("zb", zb, "gz", 1)],
        "za": [("za", za, "gz", 0)],
        "ta": [("ta", ta, "ta", 0)],
        "x": [("xa", value, "xy", 0)],
    }
    if lax.axis_size("xy") > 2:
        plan["x"].append(("xb", value, "xy", 1))
    plan = [entry for key in order for entry in plan[key]]
    for key, piece, axis, offset in plan:
        sent[key] = exchange(piece, axis, offset)
    return [sent[k] for k in ("xa", "xb") if k in sent], sent


def shards(right_side, link_blocks):
    b = right_side.reshape(S, VEC)
    links = link_blocks.reshape(link_blocks.shape[3:])
    links = pltpu.with_memory_space_constraint(links, pltpu.VMEM)
    n_x = 1 if lax.axis_size("xy") == 2 else 2
    devices = lax.axis_size("xy") * lax.axis_size("gz") * lax.axis_size("ta")

    faces = call(faces_body, FACES, (), FIRST_COST)(b)
    xs, sent = halo(b, faces, ORDERS[0])
    part, b_t = local_part(n_x, False)(b, *xs, links)
    for edge in EDGES[0][:-1]:
        part = add_edge(edge, b, sent[edge], links, part)
    edge = EDGES[0][-1]
    u_t, u, *faces = call(
        first_body(edge), ((VEC, S), (S, VEC)) + FACES, EDGE_SCRATCH
    )(b, sent[edge], links, part)
    xs, sent = halo(u, faces, ORDERS[1])
    part, b_rot, u_rot = local_part(n_x, True)(u, *xs, links, b)
    for edge in EDGES[1][:-1]:
        part = add_edge(edge, u, sent[edge], links, part)
    edge = EDGES[1][-1]
    w_t, sums = call(
        lambda *refs: second_body(edge, *refs), ((VEC, S), (devices, 1, S)), EDGE_SCRATCH + (TABLE,)
    )(u, sent[edge], links, part, u_t, b_t)
    sums = lax.all_to_all(sums, AXES, 0, 0)
    sol, res = call(final_body, ((S, VEC),) * 2, FINAL_SCRATCH, None, pl.ANY)(
        sums, b, b_rot, b_t, u, u_rot, u_t, w_t
    )
    return sol.reshape(right_side.shape), res.reshape(right_side.shape)


def solution(mesh):
    return jax.shard_map(
        shards,
        mesh=mesh,
        in_specs=(
            P("xy", "gz", "ta", None, None),
            P("xy", "gz", "ta", None, None, None, None, None),
        ),
        out_specs=(P("xy", "gz", "ta", None, None), P("xy", "gz", "ta", None, None)),
        check_vma=False,
    )
```

```python
import jax
import jax.numpy as jnp
from jax import lax
from jax.experimental import pallas as pl
from jax.experimental.pallas import tpu as pltpu
from jax.sharding import PartitionSpec as P


DOF = 32
RHS = 2
CX = 1
NY = 8
CZ = 2
CT = 8
S = CX * NY * CZ * CT
VEC = RHS * 2 * DOF
SUB = 8
TILES = DOF // SUB
AXES = ("xy", "gz", "ta")

mass_shift = 4.0
epsilon = 1e-06
f32 = jnp.float32
LOCAL_UNROLL = True
EDGES = (("tb", "zb", "ta", "za"), ("zb", "za", "tb", "ta"))
ORDERS = (("tb", "x", "zb", "ta", "za"), ("zb", "x", "za", "tb", "ta"))
FIRST_COST = 20_000_000_000

PARAMS = pltpu.CompilerParams(vmem_limit_bytes=12 * 1024 * 1024)


def call(body, outs, scratch=(), cost=None, space=pltpu.VMEM):
    if cost is not None:
        cost = pl.CostEstimate(flops=cost, bytes_accessed=0, transcendentals=0)
    return pl.pallas_call(
        body,
        out_shape=[jax.ShapeDtypeStruct(o, f32) for o in outs],
        out_specs=[pl.BlockSpec(memory_space=space)] * len(outs),
        scratch_shapes=list(scratch),
        compiler_params=PARAMS,
        cost_estimate=cost,
    )


def swap_halves(axis, first, second):
    odd = lax.axis_index(axis) % 2 == 1
    return jnp.where(odd, second, first), jnp.where(odd, first, second)


def write_faces(src_ref, za_ref, zb_ref, ta_ref, tb_ref):
    pairs = src_ref[...].reshape(NY, CZ * CT, VEC)
    low = pairs[:, :CT].reshape(NY * CT, VEC)
    high = pairs[:, (CZ - 1) * CT :].reshape(NY * CT, VEC)
    za_ref[...], zb_ref[...] = swap_halves("gz", high, low)
    rows = S // CT
    low = src_ref[pl.ds(0, rows, stride=CT), :]
    high = src_ref[pl.ds(CT - 1, rows, stride=CT), :]
    ta_ref[...], tb_ref[...] = swap_halves("ta", high, low)


FACES = ((NY * CT, VEC), (NY * CT, VEC), (S // CT, VEC), (S // CT, VEC))


def faces_body(src_ref, *outs):
    write_faces(src_ref, *outs)


def multiply(fields, links, groups, red, out, add=None, unroll=False):
    def chunk(cb, carry):
        acc = [None] * (2 * RHS * SUB)
        for field, dirs in groups:
            for tile in range(TILES):
                x = [
                    fields[field, part * DOF + tile * SUB : part * DOF + (tile + 1) * SUB, :]
                    for part in range(2 * RHS)
                ]
                rows = pl.ds(tile * SUB, SUB)
                for c in range(SUB):
                    lr = links[dirs[0], 0, cb * SUB + c, rows, :]
                    li = links[dirs[0], 1, cb * SUB + c, rows, :]
                    for k in dirs[1:]:
                        lr = lr + links[k, 0, cb * SUB + c, rows, :]
                        li = li + links[k, 1, cb * SUB + c, rows, :]
                    for r in range(RHS):
                        re = lr * x[2 * r] - li * x[2 * r + 1]
                        im = lr * x[2 * r + 1] + li * x[2 * r]
                        for part, value in ((2 * r, re), (2 * r + 1, im)):
                            slot = part * SUB + c
                            acc[slot] = value if acc[slot] is None else acc[slot] + value
        for slot, value in enumerate(acc):
            red[slot * SUB : (slot + 1) * SUB, :] = value
        for part in range(2 * RHS):
            total = red[pl.ds(part * SUB * SUB, SUB, stride=SUB), :]
            for d in range(1, SUB):
                total = total + red[pl.ds(part * SUB * SUB + d, SUB, stride=SUB), :]
            where = pl.ds(pl.multiple_of(part * DOF + cb * SUB, SUB), SUB)
            if add is not None:
                total = total + add[where, :]
            out[where, :] = total
        return carry

    lax.fori_loop(0, TILES, chunk, 0, unroll=unroll)


RED = pltpu.VMEM((2 * RHS * SUB * SUB, S), f32)


def assemble_z(own, edge, plus):
    blocks = own.reshape(NY, CZ * CT, VEC)
    edge = edge.reshape(NY, CT, VEC)
    up = jnp.concatenate([blocks[:, CT:], edge], axis=1)
    down = jnp.concatenate([edge, blocks[:, : (CZ - 1) * CT]], axis=1)
    return jnp.where(plus, up, down).reshape(S, VEC).T


def assemble_t(own, edge, plus, pad):
    rows = S // CT
    step = 3 * CT
    for i in range(rows):
        pad[i * step + CT : i * step + 2 * CT, :] = own[i * CT : (i + 1) * CT, :]
    pad[pl.ds(CT - 1, rows, stride=step), :] = edge
    pad[pl.ds(2 * CT, rows, stride=step), :] = edge
    pieces = []
    for i in range(rows):
        up = pad[i * step + CT + 1 : i * step + 2 * CT + 1, :]
        down = pad[i * step + CT - 1 : i * step + 2 * CT - 1, :]
        pieces.append(jnp.where(plus, up, down))
    return jnp.concatenate(pieces, axis=0).T


PAD = pltpu.VMEM((3 * S, VEC), f32)


def edge_part(edge, src, piece, links, part, out_t, fields, red, pad):
    axis, which = ("gz" if edge[0] == "z" else "ta"), (1 if edge[1] == "b" else 0)
    down = (lax.axis_index(axis) + which) % 2
    if axis == "gz":
        fields[0] = assemble_z(src[...], piece[...], down == 0)
        first = 5
    else:
        fields[0] = assemble_t(src[...], piece[...], down == 0, pad)
        first = 7
    multiply(fields, links, ((0, (first + down,)),), red, out_t, part, True)


EDGE_SCRATCH = (pltpu.VMEM((1, VEC, S), f32), RED, PAD)


def add_edge(edge, *args):
    body = lambda *refs: edge_part(edge, *refs)
    return call(body, ((VEC, S),), EDGE_SCRATCH)(*args)[0]


def local_part(n_x, second):
    def body(src, *refs):
        xs = [x[...] for x in refs[:n_x]]
        if n_x == 2:
            xs = swap_halves("xy", *xs)
        links, part = refs[n_x : n_x + 2]
        fields, red = refs[-2:]
        if second:
            fields[0] = src[...]
        else:
            fields[0] = src[...].T
            refs[n_x + 2][...] = fields[0]
        step = CZ * CT
        fields[1] = pltpu.roll(fields[0], S - step, 1)
        fields[2] = pltpu.roll(fields[0], step, 1)
        for i, x in enumerate(xs):
            fields[3 + i] = x.T
        dirs = ((0, (0,)), (1, (3,)), (2, (4,)))
        dirs += ((3, (1, 2)),) if n_x == 1 else ((3, (1,)), (4, (2,)))
        multiply(fields, links, dirs, red, part, None, LOCAL_UNROLL)

    outs = ((VEC, S),) * (1 if second else 2)
    return call(body, outs, (pltpu.VMEM((3 + n_x, VEC, S), f32), RED))


def first_body(edge):
    def body(src, piece, links, part, out_t, out, *refs):
        faces, scratch = refs[:4], refs[4:]
        edge_part(edge, src, piece, links, part, out_t, *scratch)
        out[...] = out_t[...].T
        write_faces(out, *faces)

    return body


def halves(ref, r):
    top = 2 * r * DOF
    return ref[top : top + DOF, :], ref[top + DOF : top + 2 * DOF, :]


def column(values):
    return jnp.sum(values, axis=0, keepdims=True)


def square(u):
    return [column(u[0] * u[0] + u[1] * u[1])]


def inner(u, w):
    return [column(u[0] * w[0] + u[1] * w[1]), column(u[0] * w[1] - u[1] * w[0])]


TERMS = 9
TABLE = pltpu.VMEM((-(-TERMS * RHS // SUB) * SUB, S), f32)


def slots(shape):
    row = lax.broadcasted_iota(jnp.int32, shape, 0)
    lane = lax.broadcasted_iota(jnp.int32, shape, 1)
    r = sum((row >= TERMS * k).astype(jnp.int32) for k in range(1, RHS))
    return (lane == (row - r * TERMS) * SUB + r) & (row < RHS * TERMS)


def second_body(edge, src, first_t, piece, links, part, zero_t, out_t, sums, *refs):
    table, scratch = refs[-1], refs[:-1]
    edge_part(edge, src, piece, links, part, out_t, *scratch)
    table[...] = jnp.zeros_like(table)
    for r in range(RHS):
        b, u, w = halves(zero_t, r), halves(first_t, r), halves(out_t, r)
        rows = square(b) + inner(b, u) + square(u) + inner(b, w) + inner(u, w) + square(w)
        for i, row in enumerate(rows):
            table[r * TERMS + i : r * TERMS + i + 1, :] = row
    total = jnp.sum(table[...], axis=1, keepdims=True)
    total = column(jnp.where(slots(table.shape), total, 0.0))
    sums[...] = jnp.broadcast_to(total[None], sums.shape)


def times(u, w):
    return (u[0] * w[0] - u[1] * w[1], u[0] * w[1] + u[1] * w[0])


def conj_times(u, w):
    return (u[0] * w[0] + u[1] * w[1], u[0] * w[1] - u[1] * w[0])


def plus(u, w):
    return (u[0] + w[0], u[1] + w[1])


def minus(u, w):
    return (u[0] - w[0], u[1] - w[1])


def scaled(s, u):
    return (s * u[0], s * u[1])


def norm2(u):
    return u[0] * u[0] + u[1] * u[1]


def coefficients(bb, bu, uu, bw, uw, ww):
    m = mass_shift
    inv = 1.0 / (bb + epsilon)
    tiny = epsilon * inv
    h00 = scaled(inv, (bu[0] + m * bb, bu[1]))
    q = (inv * bu[0] - m * tiny, inv * bu[1])
    pp = uu - 2.0 * conj_times(q, bu)[0] + norm2(q) * bb
    pp = jnp.maximum(pp, 0.0)
    s = pp * inv
    eta = s + epsilon
    bp = scaled(tiny, (bu[0] + m * bb, bu[1]))
    blp = minus(bw, times(q, bu))
    plp = minus(minus(uw, scaled(uu, q)), conj_times(q, bw))
    plp = plus(plp, scaled(norm2(q), bu))
    lplp = ww - 2.0 * conj_times(q, uw)[0] + norm2(q) * uu
    h01 = scaled(inv, plus(scaled(m, bp), blp))
    h11 = scaled(inv, (m * pp + plp[0], plp[1]))
    dp = inv * (m * m * pp + 2.0 * m * plp[0] + lplp)
    inv_eta = 1.0 / eta
    a00 = norm2(h00) + eta
    a01 = plus(conj_times(h00, h01), h11)
    cross = times(conj_times(h01, h11), bp)[0] * inv * inv_eta
    a11 = dp - norm2(h01) * tiny - norm2(h11) * (epsilon * inv_eta * inv_eta)
    a11 = a11 + 2.0 * cross + eta * epsilon
    inv00 = 1.0 / a00
    pivot = jnp.maximum(a11 - norm2(a01) * inv00, eta * epsilon)
    r0 = (h00[0], -h00[1])
    r1 = (h01[0], -h01[1])
    t = scaled(1.0 / pivot, minus(r1, scaled(inv00, conj_times(a01, r0))))
    y = scaled(inv00, minus(r0, times(a01, t)))
    return minus(y, times(t, q)), t


def final_body(sums, zero_t, first_t, second_t, sol, res, sol_stage, res_stage, sems):
    total = jnp.broadcast_to(jnp.sum(sums[...], axis=0), (SUB, S))
    row = lax.broadcasted_iota(jnp.int32, (SUB, S), 0)
    lane = lax.broadcasted_iota(jnp.int32, (SUB, S), 1)
    v = []
    for i in range(TERMS):
        value = jnp.sum(jnp.where(lane == i * SUB + row, total, 0.0), axis=1, keepdims=True)
        v.append(jnp.broadcast_to(value, (SUB, S)))
    a, t = coefficients(v[0], (v[1], v[2]), v[3], (v[4], v[5]), (v[6], v[7]), v[8])
    keep = (1.0 - mass_shift * a[0], -mass_shift * a[1])
    mixed = plus(scaled(mass_shift, t), a)
    sol_rows = []
    res_rows = []
    for r in range(RHS):
        at = lambda u: (u[0][r : r + 1, :], u[1][r : r + 1, :])
        b, u, w = halves(zero_t, r), halves(first_t, r), halves(second_t, r)
        sol_rows += list(plus(times(at(a), b), times(at(t), u)))
        res_rows += list(minus(minus(times(at(keep), b), times(at(mixed), u)), times(at(t), w)))
    sol_stage[...] = jnp.concatenate(sol_rows, axis=0).T
    sol_copy = pltpu.make_async_copy(sol_stage, sol, sems.at[0])
    sol_copy.start()
    res_stage[...] = jnp.concatenate(res_rows, axis=0).T
    res_copy = pltpu.make_async_copy(res_stage, res, sems.at[1])
    res_copy.start()
    sol_copy.wait()
    res_copy.wait()


FINAL_SCRATCH = (
    pltpu.VMEM((S, VEC), f32),
    pltpu.VMEM((S, VEC), f32),
    pltpu.SemaphoreType.DMA((2,)),
)


def exchange(value, axis, offset):
    n = lax.axis_size(axis)
    if n % 2:
        raise ValueError("odd axis " + axis)
    return lax.ppermute(
        value, axis, [(i, (i + 1 if (i - offset) % 2 == 0 else i - 1) % n) for i in range(n)]
    )


def halo(value, faces, order):
    za, zb, ta, tb = faces
    sent = {}
    plan = {
        "tb": [("tb", tb, "ta", 1)],
        "zb": [("zb", zb, "gz", 1)],
        "za": [("za", za, "gz", 0)],
        "ta": [("ta", ta, "ta", 0)],
        "x": [("xa", value, "xy", 0)],
    }
    if lax.axis_size("xy") > 2:
        plan["x"].append(("xb", value, "xy", 1))
    plan = [entry for key in order for entry in plan[key]]
    for key, piece, axis, offset in plan:
        sent[key] = exchange(piece, axis, offset)
    return [sent[k] for k in ("xa", "xb") if k in sent], sent


def shards(right_side, link_blocks):
    b = right_side.reshape(S, VEC)
    links = link_blocks.reshape(link_blocks.shape[3:])
    links = pltpu.with_memory_space_constraint(links, pltpu.VMEM)
    n_x = 1 if lax.axis_size("xy") == 2 else 2
    devices = lax.axis_size("xy") * lax.axis_size("gz") * lax.axis_size("ta")

    faces = call(faces_body, FACES, (), FIRST_COST)(b)
    xs, sent = halo(b, faces, ORDERS[0])
    part, b_t = local_part(n_x, False)(b, *xs, links)
    for edge in EDGES[0][:-1]:
        part = add_edge(edge, b, sent[edge], links, part)
    edge = EDGES[0][-1]
    u_t, u, *faces = call(
        first_body(edge), ((VEC, S), (S, VEC)) + FACES, EDGE_SCRATCH
    )(b, sent[edge], links, part)
    xs, sent = halo(u, faces, ORDERS[1])
    (part,) = local_part(n_x, True)(u_t, *xs, links)
    for edge in EDGES[1][:-1]:
        part = add_edge(edge, u, sent[edge], links, part)
    edge = EDGES[1][-1]
    w_t, sums = call(
        lambda *refs: second_body(edge, *refs),
        ((VEC, S), (devices, 1, S)),
        EDGE_SCRATCH + (TABLE,),
    )(u, u_t, sent[edge], links, part, b_t)
    sums = lax.all_to_all(sums, AXES, 0, 0)
    sol, res = call(final_body, ((S, VEC),) * 2, FINAL_SCRATCH, None, pl.ANY)(
        sums, b_t, u_t, w_t
    )
    return sol.reshape(right_side.shape), res.reshape(right_side.shape)


def solution(mesh):
    return jax.shard_map(
        shards,
        mesh=mesh,
        in_specs=(
            P("xy", "gz", "ta", None, None),
            P("xy", "gz", "ta", None, None, None, None, None),
        ),
        out_specs=(P("xy", "gz", "ta", None, None), P("xy", "gz", "ta", None, None)),
        check_vma=False,
    )
```

```python
import jax
import jax.numpy as jnp
from jax import lax
from jax.experimental import pallas as pl
from jax.experimental.pallas import tpu as pltpu
from jax.sharding import PartitionSpec as P


DOF = 32
RHS = 2
CX = 1
NY = 8
CZ = 2
CT = 8
S = CX * NY * CZ * CT
VEC = RHS * 2 * DOF
SUB = 8
TILES = DOF // SUB
AXES = ("xy", "gz", "ta")

mass_shift = 4.0
epsilon = 1e-06
f32 = jnp.float32
LOCAL_UNROLL = True
EDGES = (("tb", "zb", "ta", "za"), ("tb", "ta"))
ORDERS = (("tb", "x", "zb", "ta", "za"), ("zb", "x", "za", "tb", "ta"))
FIRST_COST = 20_000_000_000

PARAMS = pltpu.CompilerParams(vmem_limit_bytes=12 * 1024 * 1024)


def call(body, outs, scratch=(), cost=None, space=pltpu.VMEM):
    if cost is not None:
        cost = pl.CostEstimate(flops=cost, bytes_accessed=0, transcendentals=0)
    return pl.pallas_call(
        body,
        out_shape=[jax.ShapeDtypeStruct(o, f32) for o in outs],
        out_specs=[pl.BlockSpec(memory_space=space)] * len(outs),
        scratch_shapes=list(scratch),
        compiler_params=PARAMS,
        cost_estimate=cost,
    )


def swap_halves(axis, first, second):
    odd = lax.axis_index(axis) % 2 == 1
    return jnp.where(odd, second, first), jnp.where(odd, first, second)


def write_faces(src_ref, za_ref, zb_ref, ta_ref, tb_ref):
    pairs = src_ref[...].reshape(NY, CZ * CT, VEC)
    low = pairs[:, :CT].reshape(NY * CT, VEC)
    high = pairs[:, (CZ - 1) * CT :].reshape(NY * CT, VEC)
    za_ref[...], zb_ref[...] = swap_halves("gz", high, low)
    rows = S // CT
    low = src_ref[pl.ds(0, rows, stride=CT), :]
    high = src_ref[pl.ds(CT - 1, rows, stride=CT), :]
    ta_ref[...], tb_ref[...] = swap_halves("ta", high, low)


FACES = ((NY * CT, VEC), (NY * CT, VEC), (S // CT, VEC), (S // CT, VEC))


def faces_body(src_ref, *outs):
    write_faces(src_ref, *outs)


def multiply(fields, links, groups, red, out, add=None, unroll=False):
    def chunk(cb, carry):
        acc = [None] * (2 * RHS * SUB)
        for field, dirs in groups:
            for tile in range(TILES):
                x = [
                    fields[field, part * DOF + tile * SUB : part * DOF + (tile + 1) * SUB, :]
                    for part in range(2 * RHS)
                ]
                rows = pl.ds(tile * SUB, SUB)
                for c in range(SUB):
                    lr = links[dirs[0], 0, cb * SUB + c, rows, :]
                    li = links[dirs[0], 1, cb * SUB + c, rows, :]
                    for k in dirs[1:]:
                        lr = lr + links[k, 0, cb * SUB + c, rows, :]
                        li = li + links[k, 1, cb * SUB + c, rows, :]
                    for r in range(RHS):
                        re = lr * x[2 * r] - li * x[2 * r + 1]
                        im = lr * x[2 * r + 1] + li * x[2 * r]
                        for part, value in ((2 * r, re), (2 * r + 1, im)):
                            slot = part * SUB + c
                            acc[slot] = value if acc[slot] is None else acc[slot] + value
        for slot, value in enumerate(acc):
            red[slot * SUB : (slot + 1) * SUB, :] = value
        for part in range(2 * RHS):
            total = red[pl.ds(part * SUB * SUB, SUB, stride=SUB), :]
            for d in range(1, SUB):
                total = total + red[pl.ds(part * SUB * SUB + d, SUB, stride=SUB), :]
            where = pl.ds(pl.multiple_of(part * DOF + cb * SUB, SUB), SUB)
            if add is not None:
                total = total + add[where, :]
            out[where, :] = total
        return carry

    lax.fori_loop(0, TILES, chunk, 0, unroll=unroll)


RED = pltpu.VMEM((2 * RHS * SUB * SUB, S), f32)


def assemble_z(own, edge, plus):
    blocks = own.reshape(NY, CZ * CT, VEC)
    edge = edge.reshape(NY, CT, VEC)
    up = jnp.concatenate([blocks[:, CT:], edge], axis=1)
    down = jnp.concatenate([edge, blocks[:, : (CZ - 1) * CT]], axis=1)
    return jnp.where(plus, up, down).reshape(S, VEC).T


def assemble_t(own, edge, plus, pad):
    rows = S // CT
    step = 3 * CT
    for i in range(rows):
        pad[i * step + CT : i * step + 2 * CT, :] = own[i * CT : (i + 1) * CT, :]
    pad[pl.ds(CT - 1, rows, stride=step), :] = edge
    pad[pl.ds(2 * CT, rows, stride=step), :] = edge
    pieces = []
    for i in range(rows):
        up = pad[i * step + CT + 1 : i * step + 2 * CT + 1, :]
        down = pad[i * step + CT - 1 : i * step + 2 * CT - 1, :]
        pieces.append(jnp.where(plus, up, down))
    return jnp.concatenate(pieces, axis=0).T


PAD = pltpu.VMEM((3 * S, VEC), f32)


def edge_part(edge, src, piece, links, part, out_t, fields, red, pad):
    axis, which = ("gz" if edge[0] == "z" else "ta"), (1 if edge[1] == "b" else 0)
    down = (lax.axis_index(axis) + which) % 2
    if axis == "gz":
        fields[0] = assemble_z(src[...], piece[...], down == 0)
        first = 5
    else:
        fields[0] = assemble_t(src[...], piece[...], down == 0, pad)
        first = 7
    multiply(fields, links, ((0, (first + down,)),), red, out_t, part, True)


EDGE_SCRATCH = (pltpu.VMEM((2, VEC, S), f32), RED, PAD)


def add_edge(edge, *args):
    body = lambda *refs: edge_part(edge, *refs)
    return call(body, ((VEC, S),), EDGE_SCRATCH)(*args)[0]


def both_z(src, zb, za, links, part, out_t, fields, red, pad):
    dirs = ()
    for at, piece in enumerate((zb, za)):
        down = (lax.axis_index("gz") + 1 - at) % 2
        fields[at] = assemble_z(src[...], piece[...], down == 0)
        dirs += ((at, (5 + down,)),)
    multiply(fields, links, dirs, red, out_t, part, True)


def local_part(n_x, second):
    def body(src, *refs):
        xs = [x[...] for x in refs[:n_x]]
        if n_x == 2:
            xs = swap_halves("xy", *xs)
        links, part = refs[n_x : n_x + 2]
        fields, red = refs[-2:]
        if second:
            fields[0] = src[...]
        else:
            fields[0] = src[...].T
            refs[n_x + 2][...] = fields[0]
        step = CZ * CT
        fields[1] = pltpu.roll(fields[0], S - step, 1)
        fields[2] = pltpu.roll(fields[0], step, 1)
        for i, x in enumerate(xs):
            fields[3 + i] = x.T
        dirs = ((0, (0,)), (1, (3,)), (2, (4,)))
        dirs += ((3, (1, 2)),) if n_x == 1 else ((3, (1,)), (4, (2,)))
        multiply(fields, links, dirs, red, part, None, LOCAL_UNROLL)

    outs = ((VEC, S),) * (1 if second else 2)
    return call(body, outs, (pltpu.VMEM((3 + n_x, VEC, S), f32), RED))


def first_body(edge):
    def body(src, piece, links, part, out_t, out, *refs):
        faces, scratch = refs[:4], refs[4:]
        edge_part(edge, src, piece, links, part, out_t, *scratch)
        out[...] = out_t[...].T
        write_faces(out, *faces)

    return body


def halves(ref, r):
    top = 2 * r * DOF
    return ref[top : top + DOF, :], ref[top + DOF : top + 2 * DOF, :]


def column(values):
    return jnp.sum(values, axis=0, keepdims=True)


def square(u):
    return [column(u[0] * u[0] + u[1] * u[1])]


def inner(u, w):
    return [column(u[0] * w[0] + u[1] * w[1]), column(u[0] * w[1] - u[1] * w[0])]


TERMS = 9
TABLE = pltpu.VMEM((-(-TERMS * RHS // SUB) * SUB, S), f32)


def slots(shape):
    row = lax.broadcasted_iota(jnp.int32, shape, 0)
    lane = lax.broadcasted_iota(jnp.int32, shape, 1)
    r = sum((row >= TERMS * k).astype(jnp.int32) for k in range(1, RHS))
    return (lane == (row - r * TERMS) * SUB + r) & (row < RHS * TERMS)


def second_body(edge, src, first_t, piece, links, part, zero_t, out_t, sums, *refs):
    table, scratch = refs[-1], refs[:-1]
    edge_part(edge, src, piece, links, part, out_t, *scratch)
    table[...] = jnp.zeros_like(table)
    for r in range(RHS):
        b, u, w = halves(zero_t, r), halves(first_t, r), halves(out_t, r)
        rows = square(b) + inner(b, u) + square(u) + inner(b, w) + inner(u, w) + square(w)
        for i, row in enumerate(rows):
            table[r * TERMS + i : r * TERMS + i + 1, :] = row
    total = jnp.sum(table[...], axis=1, keepdims=True)
    total = column(jnp.where(slots(table.shape), total, 0.0))
    sums[...] = jnp.broadcast_to(total[None], sums.shape)


def times(u, w):
    return (u[0] * w[0] - u[1] * w[1], u[0] * w[1] + u[1] * w[0])


def conj_times(u, w):
    return (u[0] * w[0] + u[1] * w[1], u[0] * w[1] - u[1] * w[0])


def plus(u, w):
    return (u[0] + w[0], u[1] + w[1])


def minus(u, w):
    return (u[0] - w[0], u[1] - w[1])


def scaled(s, u):
    return (s * u[0], s * u[1])


def norm2(u):
    return u[0] * u[0] + u[1] * u[1]


def coefficients(bb, bu, uu, bw, uw, ww):
    m = mass_shift
    inv = 1.0 / (bb + epsilon)
    tiny = epsilon * inv
    h00 = scaled(inv, (bu[0] + m * bb, bu[1]))
    q = (inv * bu[0] - m * tiny, inv * bu[1])
    pp = uu - 2.0 * conj_times(q, bu)[0] + norm2(q) * bb
    pp = jnp.maximum(pp, 0.0)
    s = pp * inv
    eta = s + epsilon
    bp = scaled(tiny, (bu[0] + m * bb, bu[1]))
    blp = minus(bw, times(q, bu))
    plp = minus(minus(uw, scaled(uu, q)), conj_times(q, bw))
    plp = plus(plp, scaled(norm2(q), bu))
    lplp = ww - 2.0 * conj_times(q, uw)[0] + norm2(q) * uu
    h01 = scaled(inv, plus(scaled(m, bp), blp))
    h11 = scaled(inv, (m * pp + plp[0], plp[1]))
    dp = inv * (m * m * pp + 2.0 * m * plp[0] + lplp)
    inv_eta = 1.0 / eta
    a00 = norm2(h00) + eta
    a01 = plus(conj_times(h00, h01), h11)
    cross = times(conj_times(h01, h11), bp)[0] * inv * inv_eta
    a11 = dp - norm2(h01) * tiny - norm2(h11) * (epsilon * inv_eta * inv_eta)
    a11 = a11 + 2.0 * cross + eta * epsilon
    inv00 = 1.0 / a00
    pivot = jnp.maximum(a11 - norm2(a01) * inv00, eta * epsilon)
    r0 = (h00[0], -h00[1])
    r1 = (h01[0], -h01[1])
    t = scaled(1.0 / pivot, minus(r1, scaled(inv00, conj_times(a01, r0))))
    y = scaled(inv00, minus(r0, times(a01, t)))
    return minus(y, times(t, q)), t


def final_body(sums, zero_t, first_t, second_t, sol, res, sol_stage, res_stage, sems):
    total = jnp.broadcast_to(jnp.sum(sums[...], axis=0), (SUB, S))
    row = lax.broadcasted_iota(jnp.int32, (SUB, S), 0)
    lane = lax.broadcasted_iota(jnp.int32, (SUB, S), 1)
    v = []
    for i in range(TERMS):
        value = jnp.sum(jnp.where(lane == i * SUB + row, total, 0.0), axis=1, keepdims=True)
        v.append(jnp.broadcast_to(value, (SUB, S)))
    a, t = coefficients(v[0], (v[1], v[2]), v[3], (v[4], v[5]), (v[6], v[7]), v[8])
    keep = (1.0 - mass_shift * a[0], -mass_shift * a[1])
    mixed = plus(scaled(mass_shift, t), a)
    sol_rows = []
    res_rows = []
    for r in range(RHS):
        at = lambda u: (u[0][r : r + 1, :], u[1][r : r + 1, :])
        b, u, w = halves(zero_t, r), halves(first_t, r), halves(second_t, r)
        sol_rows += list(plus(times(at(a), b), times(at(t), u)))
        res_rows += list(minus(minus(times(at(keep), b), times(at(mixed), u)), times(at(t), w)))
    sol_stage[...] = jnp.concatenate(sol_rows, axis=0).T
    sol_copy = pltpu.make_async_copy(sol_stage, sol, sems.at[0])
    sol_copy.start()
    res_stage[...] = jnp.concatenate(res_rows, axis=0).T
    res_copy = pltpu.make_async_copy(res_stage, res, sems.at[1])
    res_copy.start()
    sol_copy.wait()
    res_copy.wait()


FINAL_SCRATCH = (
    pltpu.VMEM((S, VEC), f32),
    pltpu.VMEM((S, VEC), f32),
    pltpu.SemaphoreType.DMA((2,)),
)


def exchange(value, axis, offset):
    n = lax.axis_size(axis)
    if n % 2:
        raise ValueError("odd axis " + axis)
    return lax.ppermute(
        value, axis, [(i, (i + 1 if (i - offset) % 2 == 0 else i - 1) % n) for i in range(n)]
    )


def halo(value, faces, order):
    za, zb, ta, tb = faces
    sent = {}
    plan = {
        "tb": [("tb", tb, "ta", 1)],
        "zb": [("zb", zb, "gz", 1)],
        "za": [("za", za, "gz", 0)],
        "ta": [("ta", ta, "ta", 0)],
        "x": [("xa", value, "xy", 0)],
    }
    if lax.axis_size("xy") > 2:
        plan["x"].append(("xb", value, "xy", 1))
    plan = [entry for key in order for entry in plan[key]]
    for key, piece, axis, offset in plan:
        sent[key] = exchange(piece, axis, offset)
    return [sent[k] for k in ("xa", "xb") if k in sent], sent


def shards(right_side, link_blocks):
    b = right_side.reshape(S, VEC)
    links = link_blocks.reshape(link_blocks.shape[3:])
    links = pltpu.with_memory_space_constraint(links, pltpu.VMEM)
    n_x = 1 if lax.axis_size("xy") == 2 else 2
    devices = lax.axis_size("xy") * lax.axis_size("gz") * lax.axis_size("ta")

    faces = call(faces_body, FACES, (), FIRST_COST)(b)
    xs, sent = halo(b, faces, ORDERS[0])
    part, b_t = local_part(n_x, False)(b, *xs, links)
    for edge in EDGES[0][:-1]:
        part = add_edge(edge, b, sent[edge], links, part)
    edge = EDGES[0][-1]
    u_t, u, *faces = call(
        first_body(edge), ((VEC, S), (S, VEC)) + FACES, EDGE_SCRATCH
    )(b, sent[edge], links, part)
    xs, sent = halo(u, faces, ORDERS[1])
    (part,) = local_part(n_x, True)(u_t, *xs, links)
    (part,) = call(both_z, ((VEC, S),), EDGE_SCRATCH)(
        u, sent["zb"], sent["za"], links, part
    )
    for edge in EDGES[1][:-1]:
        part = add_edge(edge, u, sent[edge], links, part)
    edge = EDGES[1][-1]
    w_t, sums = call(
        lambda *refs: second_body(edge, *refs),
        ((VEC, S), (devices, 1, S)),
        EDGE_SCRATCH + (TABLE,),
    )(u, u_t, sent[edge], links, part, b_t)
    sums = lax.all_to_all(sums, AXES, 0, 0)
    sol, res = call(final_body, ((S, VEC),) * 2, FINAL_SCRATCH, None, pl.ANY)(
        sums, b_t, u_t, w_t
    )
    return sol.reshape(right_side.shape), res.reshape(right_side.shape)


def solution(mesh):
    return jax.shard_map(
        shards,
        mesh=mesh,
        in_specs=(
            P("xy", "gz", "ta", None, None),
            P("xy", "gz", "ta", None, None, None, None, None),
        ),
        out_specs=(P("xy", "gz", "ta", None, None), P("xy", "gz", "ta", None, None)),
        check_vma=False,
    )
```
